8 devices in a mesh: data: 1 (over z), stage: 8 (over y, x, core).
Axes of the slice: x: 2, y: 2, z: 1, core: 2. Of those that a mesh axis runs over, the one named last changes fastest.
Arguments:
- x_init: float32 [32, 64, 64], P('data')
- h_warm: bfloat16 [7, 32, 64, 384], P(None, 'data')
- w_lat: bfloat16 [8, 64, 384], P('stage')
- w_qkv: bfloat16 [8, 384, 1152], P('stage')
- w_o: bfloat16 [8, 6, 64, 384], P('stage')
- w_up: bfloat16 [8, 384, 1536], P('stage')
- w_down: bfloat16 [8, 1536, 384], P('stage')
- w_out: bfloat16 [384, 64], replicated
- ada_mods: float32 [4, 8, 6, 384], P(None, 'stage')
- alpha_coef: float32 [4], replicated
- beta_coef: float32 [4], replicated
Outputs:
- output 1: float32 [32, 64, 64], P('data')
- output 2: bfloat16 [8, 32, 64, 384], P('stage', 'data')
All inputs are finite; a program needn't handle non-finite values.
Results may differ from the reference program's by a relative error of at most 0.02.
Values are sent between devices in bfloat16 or wider.
A program may use at most 1 GiB of HBM per device.

```python
import jax
import jax.numpy as jnp
from jax import lax

D = 384
HEADS = 6
TOKENS = 64
CH = 64
BATCH = 32
BLOCKS_STAGE = 1
STEPS = 4
STAGES = 8

LAYERS = STAGES * BLOCKS_STAGE
HEAD = D // HEADS


def setup_inputs(seed: int = 0, part: int = 0) -> dict:
    shared_keys = jax.random.split(jax.random.key(seed), 9)
    part_keys = jax.random.split(jax.random.fold_in(jax.random.key(seed + 1), part), 2)
    x_init = jax.random.normal(part_keys[0], (BATCH, TOKENS, CH), jnp.float32)
    h_warm = jax.random.normal(part_keys[1], (STAGES - 1, BATCH, TOKENS, D), jnp.float32).astype(jnp.bfloat16)
    w_lat = (jax.random.normal(shared_keys[0], (STAGES, CH, D), jnp.float32) * CH ** -0.5).astype(jnp.bfloat16)
    w_qkv = (jax.random.normal(shared_keys[1], (LAYERS, D, 3 * D), jnp.float32) * (1.5 * D ** -0.5)).astype(jnp.bfloat16)
    w_o = (jax.random.normal(shared_keys[2], (LAYERS, HEADS, HEAD, D), jnp.float32) * D ** -0.5).astype(jnp.bfloat16)
    w_up = (jax.random.normal(shared_keys[3], (LAYERS, D, 4 * D), jnp.float32) * D ** -0.5).astype(jnp.bfloat16)
    w_down = (jax.random.normal(shared_keys[4], (LAYERS, 4 * D, D), jnp.float32) * (4 * D) ** -0.5).astype(jnp.bfloat16)
    w_out = (jax.random.normal(shared_keys[5], (D, CH), jnp.float32) * D ** -0.5).astype(jnp.bfloat16)
    mod_base = jnp.array([0.0, 0.0, 1.0, 0.0, 0.0, 0.6], jnp.float32)[:, None]
    ada_mods = mod_base + 0.3 * jax.random.normal(shared_keys[6], (STEPS, LAYERS, 6, D), jnp.float32)
    alpha_coef = jax.random.uniform(shared_keys[7], (STEPS,), jnp.float32, 0.7, 1.0)
    beta_coef = -jax.random.uniform(shared_keys[8], (STEPS,), jnp.float32, 0.3, 0.6)
    return {'x_init': x_init, 'h_warm': h_warm, 'w_lat': w_lat, 'w_qkv': w_qkv, 'w_o': w_o, 'w_up': w_up, 'w_down': w_down, 'w_out': w_out, 'ada_mods': ada_mods, 'alpha_coef': alpha_coef, 'beta_coef': beta_coef}


def layer_norm(h_cur):
    row_mean = jnp.mean(h_cur, axis=-1, keepdims=True)
    centered = h_cur - row_mean
    row_var = jnp.mean(centered * centered, axis=-1, keepdims=True)
    return centered * lax.rsqrt(row_var + 1e-6)


def dit_block(h_cur, w_qkv, w_o, w_up, w_down, mod_vec):
    batch_size, tokens = h_cur.shape[0], h_cur.shape[1]
    u_attn = (layer_norm(h_cur) * (1.0 + mod_vec[1]) + mod_vec[0]).astype(jnp.bfloat16)
    qkv_proj = jnp.einsum('bnd,de->bne', u_attn.astype(jnp.float32), w_qkv.astype(jnp.float32)).astype(jnp.bfloat16)
    qkv_proj = qkv_proj.reshape(batch_size, tokens, 3, HEADS, HEAD).astype(jnp.float32)
    scores = jnp.einsum('bqhd,bkhd->bhqk', qkv_proj[:, :, 0], qkv_proj[:, :, 1]) * HEAD ** -0.5
    attn_probs = jax.nn.softmax(scores, axis=-1).astype(jnp.bfloat16).astype(jnp.float32)
    attn_out = jnp.einsum('bhqk,bkhd->bqhd', attn_probs, qkv_proj[:, :, 2]).astype(jnp.bfloat16).astype(jnp.float32)
    h_cur = h_cur + mod_vec[2] * jnp.einsum('bqhd,hde->bqe', attn_out, w_o.astype(jnp.float32))
    u_mlp = (layer_norm(h_cur) * (1.0 + mod_vec[4]) + mod_vec[3]).astype(jnp.bfloat16)
    hidden = jax.nn.gelu(jnp.einsum('bnd,df->bnf', u_mlp.astype(jnp.float32), w_up.astype(jnp.float32)), approximate=True).astype(jnp.bfloat16)
    return h_cur + mod_vec[5] * jnp.einsum('bnf,fd->bnd', hidden.astype(jnp.float32), w_down.astype(jnp.float32))


def run_stage(h_cur, weights_s, mods_s):
    def one_block(carry_h, block_in):
        w_qkv, w_o, w_up, w_down, mod_vec = block_in
        return dit_block(carry_h, w_qkv, w_o, w_up, w_down, mod_vec), None
    h_out, _ = lax.scan(one_block, h_cur, weights_s + (mods_s,))
    return h_out


def reference(x_init, h_warm, w_lat, w_qkv, w_o, w_up, w_down, w_out, ada_mods, alpha_coef, beta_coef):
    stage_w = tuple(weight.reshape((STAGES, BLOCKS_STAGE) + weight.shape[1:]) for weight in (w_qkv, w_o, w_up, w_down))
    stage_mods = ada_mods.reshape(STEPS, STAGES, BLOCKS_STAGE, 6, D)
    zero_slot = jnp.zeros((1, BATCH, TOKENS, D), jnp.bfloat16)
    prev_init = jnp.concatenate([h_warm, zero_slot], axis=0)

    def one_step(carry, step_in):
        x_cur, prev_out = carry
        mods_t, alpha_t, beta_t = step_in
        stale_in = jnp.concatenate([zero_slot, prev_out[:-1]], axis=0)
        x_lat = x_cur.astype(jnp.bfloat16).astype(jnp.float32)

        def one_stage(stage_in):
            stale_s, lat_s, weights_s, mods_s = stage_in
            h_cur = stale_s.astype(jnp.float32) + jnp.einsum('bnc,cd->bnd', x_lat, lat_s.astype(jnp.float32))
            return run_stage(h_cur, weights_s, mods_s).astype(jnp.bfloat16)

        stage_out = lax.map(one_stage, (stale_in, w_lat, stage_w, mods_t))
        eps_pred = jnp.einsum('bnd,dc->bnc', stage_out[STAGES - 1].astype(jnp.float32), w_out.astype(jnp.float32))
        x_next = alpha_t * x_cur + beta_t * eps_pred
        return (x_next, stage_out), None

    (x_final, last_out), _ = lax.scan(one_step, (x_init, prev_init), (stage_mods, alpha_coef, beta_coef))
    return x_final, last_out
```

```python
import functools
import math

import jax
import jax.numpy as jnp
from jax import lax
from jax.experimental import pallas as pl
from jax.experimental.pallas import tpu as pltpu
from jax.sharding import PartitionSpec as P

MESH = pl.DeviceIdType.MESH
F32, BF16 = jnp.float32, jnp.bfloat16
MICRO = 4
GROUP = 256
TILE = 128
GELU_A = math.sqrt(2.0 / math.pi)
GELU_B = 0.044715


def dot(lhs, rhs):
    return lax.dot_general(lhs, rhs, (((1,), (0,)), ((), ())), preferred_element_type=F32)


def layer_norm(h, scale, shift):
    mean = jnp.sum(h, axis=0, keepdims=True) * (1.0 / h.shape[0])
    centered = h - mean
    var = jnp.sum(centered * centered, axis=0, keepdims=True) * (1.0 / h.shape[0])
    return centered * lax.rsqrt(var + 1e-6) * scale + shift


def kernel(dims, x_hbm, warm_hbm, wlat_hbm, wqkv_hbm, wo_hbm, wup_hbm, wdown_hbm, wout_hbm, mods_ref, alpha_ref, beta_ref,
           xo_ref, hl_ref,
           wlat_raw, wqkv_raw, wo_raw, wup_raw, wdown_raw, wout_raw, warm_raw, x_raw,
           wlat_t, wqkv_t, wo_t, wup_t, wdown_t, wout_t, modb,
           h_ref, u_ref, qkv_ref, att_ref, hid_ref, out_ref,
           b_in, x_in, b_out, x_f32, x_fin,
           load_sem, hs_sem, hr_sem, xs_sem, xr_sem, fs_sem, fr_sem):
    steps, stages, heads, head_dim, dim, micro, tm = dims
    stage = lax.axis_index('stage')
    last = stages - 1
    hidden = wup_t.shape[0]

    loads = [pltpu.make_async_copy(src, dst, load_sem.at[i]) for i, (src, dst) in enumerate((
        (x_hbm, x_raw), (wlat_hbm, wlat_raw), (wqkv_hbm, wqkv_raw), (wo_hbm, wo_raw),
        (wup_hbm, wup_raw), (wdown_hbm, wdown_raw), (wout_hbm, wout_raw)))]
    warm = pltpu.make_async_copy(warm_hbm.at[jnp.maximum(stage - 1, 0)], warm_raw, load_sem.at[7])
    for copy in loads:
        copy.start()
    warm.start()

    barrier = pltpu.get_barrier_semaphore()
    for shift in range(1, stages):
        pl.semaphore_signal(barrier, inc=1, device_id={'stage': lax.rem(stage + shift, stages)}, device_id_type=MESH)

    def mods_body(t, carry):
        for i in range(6):
            row = mods_ref[t, i:i + 1, :]
            if i in (1, 4):
                row = row + 1.0
            modb[t, i] = jnp.broadcast_to(row, (TILE, dim)).T
        return carry
    lax.fori_loop(0, steps, mods_body, 0)

    for copy in loads:
        copy.wait()
    warm.wait()
    wlat_t[...] = wlat_raw[...].T
    wqkv_t[...] = wqkv_raw[...].T
    wo_t[...] = wo_raw[...].T
    for j in range(hidden // dim):
        wup_t[j * dim:(j + 1) * dim, :] = wup_raw[:, j * dim:(j + 1) * dim].T * jnp.asarray(0.5, BF16)
        wdown_t[:, j * dim:(j + 1) * dim] = wdown_raw[j * dim:(j + 1) * dim, :].T
    wout_t[...] = wout_raw[...].T

    def init_body(m, carry):
        xt = x_raw[pl.ds(m * tm, tm), :].T
        x_f32[m] = xt
        x_in[0, m] = xt.astype(BF16)

        @pl.when(stage > 0)
        def _():
            b_in[0, m] = warm_raw[pl.ds(m * tm, tm), :].T

        @pl.when(stage == 0)
        def _():
            for t in range(steps):
                b_in[t, m] = jnp.zeros((dim, tm), BF16)
        return carry
    lax.fori_loop(0, micro, init_body, 0)

    pl.semaphore_wait(barrier, stages - 1)

    def h_copy(t, m):
        return pltpu.make_async_remote_copy(
            src_ref=b_out.at[t, m], dst_ref=b_in.at[t + 1, m], send_sem=hs_sem.at[t, m], recv_sem=hr_sem.at[t, m],
            device_id={'stage': jnp.minimum(stage + 1, last)}, device_id_type=MESH)

    def x_copy(t, m, dev):
        return pltpu.make_async_remote_copy(
            src_ref=x_in.at[t + 1, m], dst_ref=x_in.at[t + 1, m], send_sem=xs_sem.at[t, m, dev], recv_sem=xr_sem.at[t, m],
            device_id={'stage': dev}, device_id_type=MESH)

    def f_copy(m, dev):
        return pltpu.make_async_remote_copy(
            src_ref=x_fin.at[m], dst_ref=x_fin.at[m], send_sem=fs_sem.at[m, dev], recv_sem=fr_sem.at[m],
            device_id={'stage': dev}, device_id_type=MESH)

    low_half = lax.rem(lax.broadcasted_iota(jnp.int32, (head_dim, 2 * TILE), 1), TILE) < head_dim
    score_scale = head_dim ** -0.5 * math.log2(math.e)

    def attention(cols):
        zero_q = jnp.zeros((head_dim, TILE), BF16)
        zero_p = jnp.zeros((TILE, TILE), BF16)
        for hp in range(heads // 2):
            rows = slice(hp * TILE, (hp + 1) * TILE)
            q_pair = qkv_ref[hp * TILE:(hp + 1) * TILE, cols]
            k_pair = qkv_ref[dim + hp * TILE:dim + (hp + 1) * TILE, cols].T
            v_pair = qkv_ref[2 * dim + hp * TILE:2 * dim + (hp + 1) * TILE, cols]
            probs = []
            for sp in range(GROUP // TILE):
                span = slice(sp * TILE, (sp + 1) * TILE)
                q_blk = jnp.concatenate([
                    jnp.concatenate([q_pair[:head_dim, span], zero_q], axis=1),
                    jnp.concatenate([zero_q, q_pair[head_dim:, span]], axis=1)], axis=0)
                scores = dot(k_pair[span, :], q_blk)
                scores = jnp.where(low_half, scores[:head_dim], scores[head_dim:])
                top = jnp.max(scores, axis=0, keepdims=True)
                expd = jnp.exp2((scores - top) * score_scale)
                prob = expd * (1.0 / jnp.sum(expd, axis=0, keepdims=True))
                probs.append(jnp.concatenate([
                    jnp.where(low_half, prob, 0.0).astype(BF16), jnp.where(low_half, 0.0, prob).astype(BF16)], axis=0))
            for j in range(2):
                span = slice(j * TILE, (j + 1) * TILE)
                p_blk = jnp.concatenate([
                    jnp.concatenate([probs[0][:, span], zero_p], axis=1),
                    jnp.concatenate([zero_p, probs[1][:, span]], axis=1)], axis=0)
                out = dot(v_pair[j * head_dim:(j + 1) * head_dim, :], p_blk)
                att_ref[hp * TILE + j * head_dim:hp * TILE + (j + 1) * head_dim, cols] = out.astype(BF16)

    tiles = [slice(i * TILE, (i + 1) * TILE) for i in range(tm // TILE)]

    def slot_body(slot, carry):
        t, m = lax.div(slot, micro), lax.rem(slot, micro)

        @pl.when(jnp.logical_and(t > 0, stage > 0))
        def _():
            h_copy(t - 1, m).wait_recv()

        @pl.when(jnp.logical_and(t > 0, stage < last))
        def _():
            x_copy(t - 1, m, 0).wait_recv()

        h_ref[...] = b_in[t, m].astype(F32) + dot(wlat_t[...], x_in[t, m])
        for tile in tiles:
            u_ref[:, tile] = layer_norm(h_ref[:, tile], modb[t, 1], modb[t, 0]).astype(BF16)
        for j in range(3):
            rows = slice(j * dim, (j + 1) * dim)
            qkv_ref[rows, :] = dot(wqkv_t[rows, :], u_ref[...]).astype(BF16)
        for g in range(tm // GROUP):
            attention(slice(g * GROUP, (g + 1) * GROUP))
        proj = dot(wo_t[...], att_ref[...])
        for tile in tiles:
            h_new = h_ref[:, tile] + modb[t, 2] * proj[:, tile]
            h_ref[:, tile] = h_new
            u_ref[:, tile] = layer_norm(h_new, modb[t, 4], modb[t, 3]).astype(BF16)
        for j in range(hidden // GROUP):
            rows = slice(j * GROUP, (j + 1) * GROUP)
            half = dot(wup_t[rows, :], u_ref[...])
            inner = half * (half * half * (8.0 * GELU_A * GELU_B) + 2.0 * GELU_A)
            hid_ref[rows, :] = (half + half * jnp.tanh(inner)).astype(BF16)
        down = dot(wdown_t[...], hid_ref[...])
        for tile in tiles:
            out_ref[:, tile] = (h_ref[:, tile] + modb[t, 5] * down[:, tile]).astype(BF16)

        @pl.when(jnp.logical_and(t < steps - 1, stage < last))
        def _():
            b_out[t, m] = out_ref[...]
            h_copy(t, m).start()

        @pl.when(t == steps - 1)
        def _():
            hl_ref[pl.ds(m * tm, tm), :] = out_ref[...].T

        @pl.when(stage == last)
        def _():
            eps = dot(wout_t[...], out_ref[...])
            x_next = alpha_ref[t] * x_f32[m] + beta_ref[t] * eps
            x_f32[m] = x_next

            @pl.when(t < steps - 1)
            def _():
                x_in[t + 1, m] = x_next.astype(BF16)
                for dev in (5, 3, 1, 4, 2, 0, 6):
                    x_copy(t, m, dev).start()

            @pl.when(t == steps - 1)
            def _():
                x_fin[m] = x_next
                for dev in (5, 3, 1, 4, 2, 0, 6):
                    f_copy(m, dev).start()
        return carry

    lax.fori_loop(0, steps * micro, slot_body, 0)

    def finish_body(m, carry):
        @pl.when(stage < last)
        def _():
            f_copy(m, 0).wait_recv()
            for t in range(steps - 1):
                h_copy(t, m).wait_send()

        @pl.when(stage == last)
        def _():
            for dev in range(last):
                f_copy(m, dev).wait_send()
                for t in range(steps - 1):
                    x_copy(t, m, dev).wait_send()
        xo_ref[pl.ds(m * tm, tm), :] = x_fin[m].T
        return carry
    lax.fori_loop(0, micro, finish_body, 0)


def solution(mesh):
    stages = mesh.shape['stage']

    def stage_program(x_init, h_warm, w_lat, w_qkv, w_o, w_up, w_down, w_out, ada_mods, alpha_coef, beta_coef):
        batch, tokens, ch = x_init.shape
        total = batch * tokens
        steps, heads, head_dim, dim = ada_mods.shape[0], w_o.shape[1], w_o.shape[2], w_o.shape[3]
        hidden = w_up.shape[2]
        micro, tm = MICRO, total // MICRO
        dims = (steps, stages, heads, head_dim, dim, micro, tm)
        any_spec = pl.BlockSpec(memory_space=pl.ANY)
        vmem_spec = pl.BlockSpec(memory_space=pltpu.VMEM)
        smem_spec = pl.BlockSpec(memory_space=pltpu.SMEM)
        x_out, h_last = pl.pallas_call(
            functools.partial(kernel, dims),
            out_shape=(jax.ShapeDtypeStruct((total, ch), F32), jax.ShapeDtypeStruct((total, dim), BF16)),
            in_specs=[any_spec] * 8 + [vmem_spec, smem_spec, smem_spec],
            out_specs=(vmem_spec, vmem_spec),
            scratch_shapes=[
                pltpu.VMEM((ch, dim), BF16), pltpu.VMEM((dim, 3 * dim), BF16), pltpu.VMEM((dim, dim), BF16),
                pltpu.VMEM((dim, hidden), BF16), pltpu.VMEM((hidden, dim), BF16), pltpu.VMEM((dim, ch), BF16),
                pltpu.VMEM((total, dim), BF16), pltpu.VMEM((total, ch), F32),
                pltpu.VMEM((dim, ch), BF16), pltpu.VMEM((3 * dim, dim), BF16), pltpu.VMEM((dim, dim), BF16),
                pltpu.VMEM((hidden, dim), BF16), pltpu.VMEM((dim, hidden), BF16), pltpu.VMEM((ch, dim), BF16),
                pltpu.VMEM((steps, 6, dim, TILE), F32),
                pltpu.VMEM((dim, tm), F32), pltpu.VMEM((dim, tm), BF16), pltpu.VMEM((3 * dim, tm), BF16),
                pltpu.VMEM((dim, tm), BF16), pltpu.VMEM((hidden, tm), BF16), pltpu.VMEM((dim, tm), BF16),
                pltpu.VMEM((steps, micro, dim, tm), BF16), pltpu.VMEM((steps, micro, ch, tm), BF16),
                pltpu.VMEM((steps - 1, micro, dim, tm), BF16), pltpu.VMEM((micro, ch, tm), F32), pltpu.VMEM((micro, ch, tm), F32),
                pltpu.SemaphoreType.DMA((8,)),
                pltpu.SemaphoreType.DMA((steps - 1, micro)), pltpu.SemaphoreType.DMA((steps - 1, micro)),
                pltpu.SemaphoreType.DMA((steps - 1, micro, stages)), pltpu.SemaphoreType.DMA((steps - 1, micro)),
                pltpu.SemaphoreType.DMA((micro, stages)), pltpu.SemaphoreType.DMA((micro,)),
            ],
            compiler_params=pltpu.CompilerParams(collective_id=0, has_side_effects=True, vmem_limit_bytes=60 * 1024 * 1024),
        )(x_init.reshape(total, ch), h_warm.reshape(stages - 1, total, dim), w_lat.reshape(ch, dim),
          w_qkv.reshape(dim, 3 * dim), w_o.reshape(heads * head_dim, dim), w_up.reshape(dim, hidden),
          w_down.reshape(hidden, dim), w_out, ada_mods.reshape(steps, 6, dim), alpha_coef, beta_coef)
        return x_out.reshape(batch, tokens, ch), h_last.reshape(1, batch, tokens, dim)

    return jax.shard_map(stage_program, mesh=mesh,
                         in_specs=(P('data'), P(None, 'data'), P('stage'), P('stage'), P('stage'), P('stage'), P('stage'), P(), P(None, 'stage'), P(), P()),
                         out_specs=(P('data'), P('stage', 'data')), check_vma=False)
```

```python
import functools
import math

import jax
import jax.numpy as jnp
from jax import lax
from jax.experimental import pallas as pl
from jax.experimental.pallas import tpu as pltpu
from jax.sharding import PartitionSpec as P

MESH = pl.DeviceIdType.MESH
F32, BF16 = jnp.float32, jnp.bfloat16
GROUP = 256
TILE = 128
GELU_A = math.sqrt(2.0 / math.pi)
GELU_B = 0.044715


def dot(lhs, rhs):
    return lax.dot_general(lhs, rhs, (((1,), (0,)), ((), ())), preferred_element_type=F32)


def layer_norm(h, scale, shift):
    mean = jnp.sum(h, axis=0, keepdims=True) * (1.0 / h.shape[0])
    centered = h - mean
    var = jnp.sum(centered * centered, axis=0, keepdims=True) * (1.0 / h.shape[0])
    return centered * lax.rsqrt(var + 1e-6) * scale + shift


def kernel(dims, x_hbm, warm_hbm, wlat_hbm, wqkv_hbm, wo_hbm, wup_hbm, wdown_hbm, wout_ref, mods_ref, alpha_ref, beta_ref,
           xo_ref, hl_ref,
           wlat_raw, wqkv_raw, wo_raw, wup_raw, wdown_raw, warm_raw, x_raw,
           wlat_t, wqkv_t, wo_t, wup_t, wdown_t, modb,
           h_ref, hb_ref, h2_ref, h2b_ref, u_ref, u2_ref, q_ref, k_ref, v_ref, att_ref, hid_ref,
           b_in, x_in, b_out, x_out, x_f32,
           load_sem, hs_sem, hr_sem, xs_sem, xr_sem, fs_sem, fr_sem):
    steps, stages, heads, head_dim, dim, micro, tm = dims
    stage = lax.axis_index('stage')
    last = stages - 1
    hidden = wup_t.shape[0]
    slots = steps * micro
    others = (5, 3, 1, 4, 2, 0, 6)

    loads = [pltpu.make_async_copy(src, dst, load_sem.at[i]) for i, (src, dst) in enumerate((
        (x_hbm, x_raw), (wlat_hbm, wlat_raw), (wqkv_hbm, wqkv_raw), (wo_hbm, wo_raw),
        (wup_hbm, wup_raw), (wdown_hbm, wdown_raw)))]
    warm = pltpu.make_async_copy(warm_hbm.at[jnp.maximum(stage - 1, 0)], warm_raw, load_sem.at[6])
    for copy in loads:
        copy.start()
    warm.start()

    barrier = pltpu.get_barrier_semaphore()
    for shift in range(1, stages):
        pl.semaphore_signal(barrier, inc=1, device_id={'stage': lax.rem(stage + shift, stages)}, device_id_type=MESH)

    def make_mods(t):
        for i in range(6):
            row = mods_ref[i, pl.ds(t, 1), :]
            if i in (1, 4):
                row = row + 1.0
            modb[t, i] = jnp.broadcast_to(row, (TILE, dim)).T

    def make_inputs(m):
        xt = x_raw[pl.ds(m * tm, tm), :].T
        x_f32[m] = xt
        x_in[0, m] = xt.astype(BF16)

        @pl.when(stage > 0)
        def _():
            b_in[0, m] = warm_raw[pl.ds(m * tm, tm), :].T

        @pl.when(stage == 0)
        def _():
            for t in range(steps):
                b_in[t, m] = jnp.zeros((dim, tm), BF16)

    make_mods(0)
    loads[0].wait()
    warm.wait()
    make_inputs(0)
    for copy in loads[1:3]:
        copy.wait()
    wlat_t[...] = wlat_raw[...].T
    wqkv_t[...] = wqkv_raw[...].T
    for copy in loads[3:]:
        copy.wait()

    def late_weights():
        wo_t[...] = wo_raw[...].T
        for j in range(hidden // dim):
            wup_t[j * dim:(j + 1) * dim, :] = wup_raw[:, j * dim:(j + 1) * dim].T * jnp.asarray(0.5, BF16)
            wdown_t[:, j * dim:(j + 1) * dim] = wdown_raw[j * dim:(j + 1) * dim, :].T

    def h_copy(t, m):
        return pltpu.make_async_remote_copy(
            src_ref=b_out.at[t, m], dst_ref=b_in.at[t + 1, m], send_sem=hs_sem, recv_sem=hr_sem.at[t, m],
            device_id={'stage': jnp.minimum(stage + 1, last)}, device_id_type=MESH)

    def x_copy(t, m, dev):
        return pltpu.make_async_remote_copy(
            src_ref=x_out.at[t, m], dst_ref=x_in.at[t + 1, m], send_sem=xs_sem.at[dev], recv_sem=xr_sem.at[t, m],
            device_id={'stage': dev}, device_id_type=MESH)

    def f_copy(m, src, dev):
        return pltpu.make_async_remote_copy(
            src_ref=src.at[m], dst_ref=xo_ref.at[m], send_sem=fs_sem.at[dev], recv_sem=fr_sem,
            device_id={'stage': dev}, device_id_type=MESH)

    low_half = lax.rem(lax.broadcasted_iota(jnp.int32, (head_dim, 2 * TILE), 1), TILE) < head_dim
    score_scale = head_dim ** -0.5 * math.log2(math.e)
    tiles = [slice(i * TILE, (i + 1) * TILE) for i in range(tm // TILE)]
    halves = [slice(0, dim // 2), slice(dim // 2, dim)]
    zero_q = jnp.zeros((head_dim, TILE), BF16)
    zero_p = jnp.zeros((TILE, TILE), BF16)

    def step_of(slot):
        return lax.div(slot, micro), lax.rem(slot, micro)

    def attn_in(slot):
        t, m = step_of(slot)
        for rows in halves:
            h_ref[rows, :] = b_in[t, m, rows, :].astype(F32) + dot(wlat_t[rows, :], x_in[t, m])

    def attn_norm(slot):
        t, _ = step_of(slot)
        for tile in tiles:
            u_ref[:, tile] = layer_norm(h_ref[:, tile], modb[t, 1], modb[t, 0]).astype(BF16)

    def project(part, dst):
        for rows in halves:
            dst[rows, :] = dot(wqkv_t[part * dim + rows.start:part * dim + rows.stop, :], u_ref[...]).astype(BF16)

    def score_dots():
        scores = []
        for hp in range(heads // 2):
            rows = slice(hp * TILE, (hp + 1) * TILE)
            q_pair = q_ref[rows, :]
            k_pair = k_ref[rows, :].T
            for span in tiles:
                q_blk = jnp.concatenate([
                    jnp.concatenate([q_pair[:head_dim, span], zero_q], axis=1),
                    jnp.concatenate([zero_q, q_pair[head_dim:, span]], axis=1)], axis=0)
                full = dot(k_pair[span, :], q_blk)
                scores.append(jnp.where(low_half, full[:head_dim], full[head_dim:]))
        return scores

    def softmax(scores):
        top = jnp.max(scores, axis=0, keepdims=True)
        expd = jnp.exp2((scores - top) * score_scale)
        prob = expd * (1.0 / jnp.sum(expd, axis=0, keepdims=True))
        return jnp.concatenate([jnp.where(low_half, prob, 0.0).astype(BF16), jnp.where(low_half, 0.0, prob).astype(BF16)], axis=0)

    def value_dots(probs):
        for head in range(heads):
            hp, span = head // 2, tiles[head % 2]
            p_blk = jnp.concatenate([
                jnp.concatenate([probs[2 * hp][:, span], zero_p], axis=1),
                jnp.concatenate([zero_p, probs[2 * hp + 1][:, span]], axis=1)], axis=0)
            rows = slice(head * head_dim, (head + 1) * head_dim)
            att_ref[rows, :] = dot(v_ref[rows, :], p_blk).astype(BF16)

    def attn_out(slot):
        t, _ = step_of(slot)
        for rows in halves:
            proj = dot(wo_t[rows, :], att_ref[...])
            for tile in tiles:
                h2_ref[rows, tile] = hb_ref[rows, tile] + modb[t, 2, rows, :] * proj[:, tile]

    def mlp_norm(slot):
        t, _ = step_of(slot)
        for tile in tiles:
            u2_ref[:, tile] = layer_norm(h2_ref[:, tile], modb[t, 4], modb[t, 3]).astype(BF16)

    def mlp_up(j):
        rows = slice(j * GROUP, (j + 1) * GROUP)
        half = dot(wup_t[rows, :], u2_ref[...])
        inner = half * (half * half * (8.0 * GELU_A * GELU_B) + 2.0 * GELU_A)
        hid_ref[rows, :] = (half + half * jnp.tanh(inner)).astype(BF16)

    def mlp_down(slot, part):
        t, m = step_of(slot)
        cut = slice(part * hidden // 2, (part + 1) * hidden // 2)
        for rows in halves:
            down = dot(wdown_t[rows, cut], hid_ref[cut, :])
            for tile in tiles:
                if part == 0:
                    h2b_ref[rows, tile] = h2b_ref[rows, tile] + modb[t, 5, rows, :] * down[:, tile]
                else:
                    b_out[t, m, rows, tile] = (h2b_ref[rows, tile] + modb[t, 5, rows, :] * down[:, tile]).astype(BF16)

    def latent(slot):
        t, m = step_of(slot)
        eps = dot(wout_ref[...], b_out[t, m])
        x_next = alpha_ref[t] * x_f32[m] + beta_ref[t] * eps
        x_f32[m] = x_next
        x_out[t, m] = x_next.astype(BF16)
        hl_ref[pl.ds(m * tm, tm), :] = b_out[t, m].T

    def receive(slot):
        t, m = step_of(slot)

        @pl.when(jnp.logical_and(t > 0, stage > 0))
        def _():
            h_copy(t - 1, m).wait_recv()

        @pl.when(jnp.logical_and(t > 0, stage < last))
        def _():
            x_copy(t - 1, m, 0).wait_recv()

    def send_stage(slot):
        t, m = step_of(slot)

        @pl.when(jnp.logical_and(t < steps - 1, stage < last))
        def _():
            h_copy(t, m).start()

    def send_latent(slot):
        t, m = step_of(slot)

        @pl.when(jnp.logical_and(t < steps - 1, stage == last))
        def _():
            x_in[t + 1, m] = x_out[t, m]
            for dev in others:
                x_copy(t, m, dev).start()

        @pl.when(jnp.logical_and(t == steps - 1, stage == last))
        def _():
            xo_ref[m] = x_f32[m]
            for dev in (5, 3, 1, 6):
                f_copy(m, x_f32, dev).start()

    def block(attn=None, out=None, mlp=None, lat=None, extra=None):
        ups = hidden // GROUP
        if mlp is not None:
            h2b_ref[...] = h2_ref[...]
        if out is not None:
            hb_ref[...] = h_ref[...]
        if attn is not None:
            attn_in(attn)
        if lat is not None:
            latent(lat)
        if mlp is not None:
            for j in range(4):
                mlp_up(j)
        if attn is not None:
            attn_norm(attn)
            project(0, q_ref)
            project(1, k_ref)
        if mlp is not None:
            for j in range(4, ups):
                mlp_up(j)
        if attn is not None:
            scores = score_dots()
            project(2, v_ref)
        if out is not None:
            attn_out(out)
            mlp_norm(out)
        if extra is not None:
            extra()
        if mlp is not None:
            mlp_down(mlp, 0)
        if attn is not None:
            value_dots([softmax(s) for s in scores])
        if mlp is not None:
            mlp_down(mlp, 1)
            send_stage(mlp)
        if lat is not None:
            send_latent(lat)

    def whole_slot(slot):
        receive(slot)
        attn_in(slot)
        attn_norm(slot)
        project(0, q_ref)
        project(1, k_ref)
        scores = score_dots()
        project(2, v_ref)
        hb_ref[...] = h_ref[...]
        value_dots([softmax(s) for s in scores])
        attn_out(slot)
        mlp_norm(slot)
        h2b_ref[...] = h2_ref[...]
        for j in range(hidden // GROUP):
            mlp_up(j)
        mlp_down(slot, 0)
        mlp_down(slot, 1)
        latent(slot)
        send_latent(slot)

    block(attn=0, extra=late_weights)
    make_inputs(1)
    block(attn=1, out=0)
    make_inputs(2)
    pl.semaphore_wait(barrier, stages - 1)

    def slot_body(slot, carry):
        t, m = step_of(slot)
        receive(slot)
        block(slot, slot - 1, slot - 2, slot - 3)

        @pl.when(slot + 1 < micro)
        def _():
            make_inputs(slot + 1)

        @pl.when(jnp.logical_and(m == micro - 1, t < steps - 1))
        def _():
            make_mods(t + 1)
        return carry
    block(2, 1, 0)
    make_inputs(3)
    tail = slots - 2
    lax.fori_loop(3, tail, slot_body, 0)
    block(None, tail - 1, tail - 2, tail - 3)
    block(None, None, tail - 1, tail - 2)
    block(None, None, None, tail - 1)

    def tail_body(slot, carry):
        whole_slot(slot)
        return carry
    lax.fori_loop(tail, slots, tail_body, 0)

    def whole(src, dst, sem, dev):
        return pltpu.make_async_remote_copy(
            src_ref=src, dst_ref=dst, send_sem=sem, recv_sem=fr_sem, device_id={'stage': dev}, device_id_type=MESH)

    sent = pl.ds(0, steps - 1)

    @pl.when(stage < last)
    def _():
        whole(xo_ref, xo_ref, fs_sem.at[0], 0).wait_recv()
    for src, dev in ((5, 4), (3, 2), (1, 0)):
        @pl.when(stage == src)
        def _(dev=dev):
            whole(xo_ref, xo_ref, fs_sem.at[dev], dev).start()

    @pl.when(stage < last)
    def _():
        whole(b_out.at[sent], b_in.at[pl.ds(1, steps - 1)], hs_sem, jnp.minimum(stage + 1, last)).wait_send()
    for src, dev in ((5, 4), (3, 2), (1, 0)):
        @pl.when(stage == src)
        def _(dev=dev):
            whole(xo_ref, xo_ref, fs_sem.at[dev], dev).wait_send()

    @pl.when(stage == last)
    def _():
        for dev in others:
            whole(x_out.at[sent], x_in.at[pl.ds(1, steps - 1)], xs_sem.at[dev], dev).wait_send()
        for dev in (5, 3, 1, 6):
            whole(x_f32, xo_ref, fs_sem.at[dev], dev).wait_send()


def solution(mesh):
    stages = mesh.shape['stage']

    def stage_program(x_init, h_warm, w_lat, w_qkv, w_o, w_up, w_down, w_out, ada_mods, alpha_coef, beta_coef):
        batch, tokens, ch = x_init.shape
        total = batch * tokens
        steps, heads, head_dim, dim = ada_mods.shape[0], w_o.shape[1], w_o.shape[2], w_o.shape[3]
        hidden = w_up.shape[2]
        micro, tm = total // GROUP, GROUP
        dims = (steps, stages, heads, head_dim, dim, micro, tm)
        any_spec = pl.BlockSpec(memory_space=pl.ANY)
        vmem_spec = pl.BlockSpec(memory_space=pltpu.VMEM)
        smem_spec = pl.BlockSpec(memory_space=pltpu.SMEM)
        x_out, h_last = pl.pallas_call(
            functools.partial(kernel, dims),
            out_shape=(jax.ShapeDtypeStruct((micro, ch, tm), F32), jax.ShapeDtypeStruct((total, dim), BF16)),
            in_specs=[any_spec] * 7 + [vmem_spec, vmem_spec, smem_spec, smem_spec],
            out_specs=(vmem_spec, vmem_spec),
            scratch_shapes=[
                pltpu.VMEM((ch, dim), BF16), pltpu.VMEM((dim, 3 * dim), BF16), pltpu.VMEM((dim, dim), BF16),
                pltpu.VMEM((dim, hidden), BF16), pltpu.VMEM((hidden, dim), BF16),
                pltpu.VMEM((total, dim), BF16), pltpu.VMEM((total, ch), F32),
                pltpu.VMEM((dim, ch), BF16), pltpu.VMEM((3 * dim, dim), BF16), pltpu.VMEM((dim, dim), BF16),
                pltpu.VMEM((hidden, dim), BF16), pltpu.VMEM((dim, hidden), BF16),
                pltpu.VMEM((steps, 6, dim, TILE), F32),
                pltpu.VMEM((dim, tm), F32), pltpu.VMEM((dim, tm), F32), pltpu.VMEM((dim, tm), F32), pltpu.VMEM((dim, tm), F32),
                pltpu.VMEM((dim, tm), BF16), pltpu.VMEM((dim, tm), BF16),
                pltpu.VMEM((dim, tm), BF16), pltpu.VMEM((dim, tm), BF16), pltpu.VMEM((dim, tm), BF16),
                pltpu.VMEM((dim, tm), BF16), pltpu.VMEM((hidden, tm), BF16),
                pltpu.VMEM((steps, micro, dim, tm), BF16), pltpu.VMEM((steps, micro, ch, tm), BF16),
                pltpu.VMEM((steps, micro, dim, tm), BF16), pltpu.VMEM((steps, micro, ch, tm), BF16), pltpu.VMEM((micro, ch, tm), F32),
                pltpu.SemaphoreType.DMA((7,)),
                pltpu.SemaphoreType.DMA, pltpu.SemaphoreType.DMA((steps - 1, micro)),
                pltpu.SemaphoreType.DMA((stages,)), pltpu.SemaphoreType.DMA((steps - 1, micro)),
                pltpu.SemaphoreType.DMA((stages,)), pltpu.SemaphoreType.DMA,
            ],
            compiler_params=pltpu.CompilerParams(collective_id=0, has_side_effects=True, vmem_limit_bytes=60 * 1024 * 1024),
        )(x_init.reshape(total, ch), h_warm.reshape(stages - 1, total, dim), w_lat.reshape(ch, dim),
          w_qkv.reshape(dim, 3 * dim), w_o.reshape(heads * head_dim, dim), w_up.reshape(dim, hidden),
          w_down.reshape(hidden, dim), w_out.T, ada_mods.reshape(steps, 6, dim).transpose(1, 0, 2), alpha_coef, beta_coef)
        x_out = x_out.transpose(0, 2, 1)
        return x_out.reshape(batch, tokens, ch), h_last.reshape(1, batch, tokens, dim)

    return jax.shard_map(stage_program, mesh=mesh,
                         in_specs=(P('data'), P(None, 'data'), P('stage'), P('stage'), P('stage'), P('stage'), P('stage'), P(), P(None, 'stage'), P(), P()),
                         out_specs=(P('data'), P('stage', 'data')), check_vma=False)
```

```python
import functools
import math

import jax
import jax.numpy as jnp
from jax import lax
from jax.experimental import pallas as pl
from jax.experimental.pallas import tpu as pltpu
from jax.sharding import PartitionSpec as P

MESH = pl.DeviceIdType.MESH
F32, BF16 = jnp.float32, jnp.bfloat16
GROUP = 256
TILE = 128
GELU_A = math.sqrt(2.0 / math.pi)
GELU_B = 0.044715


def dot(lhs, rhs):
    return lax.dot_general(lhs, rhs, (((1,), (0,)), ((), ())), preferred_element_type=F32)


def layer_norm(src, dst, scale, shift):
    dim, tm = src.shape
    chunks = [slice(i, i + 64) for i in range(0, dim, 64)]

    def total(terms):
        part = sum(jnp.sum(term.reshape(8, 8, tm), axis=0) for term in terms)
        return jnp.sum(part, axis=0, keepdims=True) * (1.0 / dim)

    mean = total(src[rows, :] for rows in chunks)
    var = total((src[rows, :] - mean) * (src[rows, :] - mean) for rows in chunks)
    inv = lax.rsqrt(var + 1e-6)
    for rows in chunks:
        for lane in range(0, tm, TILE):
            tile = slice(lane, lane + TILE)
            dst[rows, tile] = ((src[rows, tile] - mean[:, tile]) * inv[:, tile] * scale[rows, :] + shift[rows, :]).astype(BF16)


def kernel(dims, x_hbm, warm_hbm, wlat_hbm, wqkv_hbm, wo_hbm, wup_hbm, wdown_hbm, wout_hbm, mods_hbm, alpha_ref, beta_ref,
           xo_ref, hl_ref,
           wout_ref, mods_ref, wlat_raw, wqkv_raw, wo_raw, wup_raw, wdown_raw, warm_raw, x_raw,
           wlat_t, wqkv_t, wo_t, wup_t, wdown_t, modb,
           h_ref, hb_ref, h2_ref, h2b_ref, u_ref, u2_ref, q_ref, k_ref, v_ref, att_ref, hid_ref,
           b_in, x_in, b_out, x_out, x_f32,
           load_sem, hs_sem, hr_sem, xs_sem, xr_sem, fs_sem, fr_sem):
    steps, stages, heads, head_dim, dim, micro, tm = dims
    stage = lax.axis_index('stage')
    last = stages - 1
    hidden = wup_t.shape[0]
    slots = steps * micro
    others = (5, 3, 1, 4, 2, 0, 6)

    loads = [pltpu.make_async_copy(src, dst, load_sem.at[i]) for i, (src, dst) in enumerate((
        (x_hbm, x_raw), (wlat_hbm, wlat_raw), (wqkv_hbm, wqkv_raw), (wo_hbm, wo_raw),
        (wup_hbm, wup_raw), (wdown_hbm, wdown_raw), (wout_hbm, wout_ref)))]
    mods = pltpu.make_async_copy(mods_hbm, mods_ref, load_sem.at[8])
    warm = pltpu.make_async_copy(warm_hbm.at[jnp.maximum(stage - 1, 0)], warm_raw, load_sem.at[7])
    mods.start()
    loads[0].start()
    warm.start()
    for copy in loads[1:]:
        copy.start()

    barrier = pltpu.get_barrier_semaphore()
    for shift in range(1, stages):
        pl.semaphore_signal(barrier, inc=1, device_id={'stage': lax.rem(stage + shift, stages)}, device_id_type=MESH)

    def make_mods(t):
        for i in range(6):
            for c in range(dim // TILE):
                row = mods_ref[pl.ds((t * 6 + i) * (dim // TILE) + c, 1), :]
                if i in (1, 4):
                    row = row + 1.0
                modb[t, i, c * TILE:(c + 1) * TILE, :] = jnp.broadcast_to(row, (TILE, TILE)).T

    def make_inputs(m):
        xt = x_raw[pl.ds(m * tm, tm), :].T
        x_f32[m] = xt
        x_in[0, m] = xt.astype(BF16)

        @pl.when(stage > 0)
        def _():
            b_in[0, m] = warm_raw[pl.ds(m * tm, tm), :].T

        @pl.when(stage == 0)
        def _():
            for t in range(steps):
                b_in[t, m] = jnp.zeros((dim, tm), BF16)

    mods.wait()

    def mods_body(t, carry):
        make_mods(t)
        return carry
    lax.fori_loop(0, steps, mods_body, 0)
    loads[0].wait()
    warm.wait()

    def inputs_body(m, carry):
        make_inputs(m)
        return carry
    lax.fori_loop(0, micro, inputs_body, 0)
    for copy in loads[1:3]:
        copy.wait()
    wlat_t[...] = wlat_raw[...].T
    wqkv_t[...] = wqkv_raw[...].T
    for copy in loads[3:]:
        copy.wait()

    def late_weights():
        wo_t[...] = wo_raw[...].T
        for j in range(hidden // dim):
            wup_t[j * dim:(j + 1) * dim, :] = wup_raw[:, j * dim:(j + 1) * dim].T * jnp.asarray(0.5, BF16)
            wdown_t[:, j * dim:(j + 1) * dim] = wdown_raw[j * dim:(j + 1) * dim, :].T

    def h_copy(t, m):
        return pltpu.make_async_remote_copy(
            src_ref=b_out.at[t, m], dst_ref=b_in.at[t + 1, m], send_sem=hs_sem, recv_sem=hr_sem.at[t, m],
            device_id={'stage': jnp.minimum(stage + 1, last)}, device_id_type=MESH)

    def x_copy(t, m, dev):
        return pltpu.make_async_remote_copy(
            src_ref=x_out.at[t, m], dst_ref=x_in.at[t + 1, m], send_sem=xs_sem.at[dev], recv_sem=xr_sem.at[t, m],
            device_id={'stage': dev}, device_id_type=MESH)

    def f_copy(m, src, dev):
        return pltpu.make_async_remote_copy(
            src_ref=src.at[m], dst_ref=xo_ref.at[m], send_sem=fs_sem.at[dev], recv_sem=fr_sem,
            device_id={'stage': dev}, device_id_type=MESH)

    low_half = lax.rem(lax.broadcasted_iota(jnp.int32, (head_dim, 2 * TILE), 1), TILE) < head_dim
    score_scale = head_dim ** -0.5 * math.log2(math.e)
    tiles = [slice(i * TILE, (i + 1) * TILE) for i in range(tm // TILE)]
    halves = [slice(0, dim // 2), slice(dim // 2, dim)]
    zero_q = jnp.zeros((head_dim, TILE), BF16)
    zero_p = jnp.zeros((TILE, TILE), BF16)

    def step_of(slot):
        return lax.div(slot, micro), lax.rem(slot, micro)

    def attn_in(slot):
        t, m = step_of(slot)
        for rows in halves:
            h_ref[rows, :] = b_in[t, m, rows, :].astype(F32) + dot(wlat_t[rows, :], x_in[t, m])

    def attn_norm(slot):
        t, _ = step_of(slot)
        layer_norm(h_ref, u_ref, modb.at[t, 1], modb.at[t, 0])

    def project(part, dst):
        for rows in halves:
            dst[rows, :] = dot(wqkv_t[part * dim + rows.start:part * dim + rows.stop, :], u_ref[...]).astype(BF16)

    def score_dots():
        scores = []
        for hp in range(heads // 2):
            rows = slice(hp * TILE, (hp + 1) * TILE)
            q_pair = q_ref[rows, :]
            k_pair = k_ref[rows, :].T
            for span in tiles:
                q_blk = jnp.concatenate([
                    jnp.concatenate([q_pair[:head_dim, span], zero_q], axis=1),
                    jnp.concatenate([zero_q, q_pair[head_dim:, span]], axis=1)], axis=0)
                full = dot(k_pair[span, :], q_blk)
                scores.append(jnp.where(low_half, full[:head_dim], full[head_dim:]))
        return scores

    def softmax(scores):
        top = jnp.max(scores, axis=0, keepdims=True)
        expd = jnp.exp2((scores - top) * score_scale)
        prob = (expd * (1.0 / jnp.sum(expd, axis=0, keepdims=True))).astype(BF16)
        nought = jnp.zeros_like(prob)
        return jnp.concatenate([jnp.where(low_half, prob, nought), jnp.where(low_half, nought, prob)], axis=0)

    def value_dots(probs):
        for head in range(heads):
            hp, span = head // 2, tiles[head % 2]
            p_blk = jnp.concatenate([
                jnp.concatenate([probs[2 * hp][:, span], zero_p], axis=1),
                jnp.concatenate([zero_p, probs[2 * hp + 1][:, span]], axis=1)], axis=0)
            rows = slice(head * head_dim, (head + 1) * head_dim)
            att_ref[rows, :] = dot(v_ref[rows, :], p_blk).astype(BF16)

    def attn_out(slot):
        t, _ = step_of(slot)
        for rows in halves:
            proj = dot(wo_t[rows, :], att_ref[...])
            for tile in tiles:
                h2_ref[rows, tile] = hb_ref[rows, tile] + modb[t, 2, rows, :] * proj[:, tile]

    def mlp_norm(slot):
        t, _ = step_of(slot)
        layer_norm(h2_ref, u2_ref, modb.at[t, 4], modb.at[t, 3])

    def mlp_up(j):
        rows = slice(j * GROUP, (j + 1) * GROUP)
        half = dot(wup_t[rows, :], u2_ref[...])
        inner = half * (half * half * (8.0 * GELU_A * GELU_B) + 2.0 * GELU_A)
        hid_ref[rows, :] = (half + half * jnp.tanh(inner)).astype(BF16)

    def mlp_down(slot, part):
        t, m = step_of(slot)
        cut = slice(part * hidden // 2, (part + 1) * hidden // 2)
        for rows in halves:
            down = dot(wdown_t[rows, cut], hid_ref[cut, :])
            for tile in tiles:
                if part == 0:
                    h2b_ref[rows, tile] = h2_ref[rows, tile] + modb[t, 5, rows, :] * down[:, tile]
                else:
                    b_out[t, m, rows, tile] = (h2b_ref[rows, tile] + modb[t, 5, rows, :] * down[:, tile]).astype(BF16)

    def latent(slot):
        t, m = step_of(slot)
        eps = dot(wout_ref[...], b_out[t, m])
        x_next = alpha_ref[t] * x_f32[m] + beta_ref[t] * eps
        x_f32[m] = x_next
        x_out[t, m] = x_next.astype(BF16)
        hl_ref[pl.ds(m * tm, tm), :] = b_out[t, m].T

    def receive(slot):
        t, m = step_of(slot)

        @pl.when(jnp.logical_and(t > 0, stage > 0))
        def _():
            h_copy(t - 1, m).wait_recv()

        @pl.when(jnp.logical_and(t > 0, stage < last))
        def _():
            x_copy(t - 1, m, 0).wait_recv()

    def send_stage(slot):
        t, m = step_of(slot)

        @pl.when(jnp.logical_and(t < steps - 1, stage < last))
        def _():
            h_copy(t, m).start()

    def send_latent(slot):
        t, m = step_of(slot)

        @pl.when(jnp.logical_and(t < steps - 1, stage == last))
        def _():
            x_in[t + 1, m] = x_out[t, m]
            for dev in others:
                x_copy(t, m, dev).start()

        @pl.when(jnp.logical_and(t == steps - 1, stage == last))
        def _():
            xo_ref[m] = x_f32[m]
            for dev in (5, 3, 1, 6):
                f_copy(m, x_f32, dev).start()

    def block(attn=None, out=None, mlp=None, lat=None, extra=None):
        ups = hidden // GROUP
        if out is not None:
            hb_ref[...] = h_ref[...]
        if attn is not None:
            attn_in(attn)
        if lat is not None:
            latent(lat)
        if mlp is not None:
            for j in range(4):
                mlp_up(j)
        if attn is not None:
            attn_norm(attn)
            project(0, q_ref)
            project(1, k_ref)
        if mlp is not None:
            for j in range(4, ups):
                mlp_up(j)
        if attn is not None:
            scores = score_dots()
            project(2, v_ref)
        if mlp is not None:
            mlp_down(mlp, 0)
        if out is not None:
            attn_out(out)
            mlp_norm(out)
        if extra is not None:
            extra()
        if attn is not None:
            value_dots([softmax(s) for s in scores])
        if mlp is not None:
            mlp_down(mlp, 1)
            send_stage(mlp)
        if lat is not None:
            send_latent(lat)

    block(attn=0, extra=late_weights)
    block(attn=1, out=0)
    pl.semaphore_wait(barrier, stages - 1)

    def slot_body(slot, carry):
        t, m = step_of(slot)
        receive(slot)
        block(slot, slot - 1, slot - 2, slot - 3)
        return carry
    block(2, 1, 0)
    lax.fori_loop(3, slots, slot_body, 0)
    block(None, slots - 1, slots - 2, slots - 3)
    block(None, None, slots - 1, slots - 2)
    block(None, None, None, slots - 1)

    def whole(src, dst, sem, dev):
        return pltpu.make_async_remote_copy(
            src_ref=src, dst_ref=dst, send_sem=sem, recv_sem=fr_sem, device_id={'stage': dev}, device_id_type=MESH)

    sent = pl.ds(0, steps - 1)

    @pl.when(stage < last)
    def _():
        whole(xo_ref, xo_ref, fs_sem.at[0], 0).wait_recv()
    for src, dev in ((5, 4), (3, 2), (1, 0)):
        @pl.when(stage == src)
        def _(dev=dev):
            whole(xo_ref, xo_ref, fs_sem.at[dev], dev).start()

    @pl.when(stage < last)
    def _():
        whole(b_out.at[sent], b_in.at[pl.ds(1, steps - 1)], hs_sem, jnp.minimum(stage + 1, last)).wait_send()
    for src, dev in ((5, 4), (3, 2), (1, 0)):
        @pl.when(stage == src)
        def _(dev=dev):
            whole(xo_ref, xo_ref, fs_sem.at[dev], dev).wait_send()

    @pl.when(stage == last)
    def _():
        for dev in others:
            whole(x_out.at[sent], x_in.at[pl.ds(1, steps - 1)], xs_sem.at[dev], dev).wait_send()
        for dev in (5, 3, 1, 6):
            whole(x_f32, xo_ref, fs_sem.at[dev], dev).wait_send()


def solution(mesh):
    stages = mesh.shape['stage']

    def stage_program(x_init, h_warm, w_lat, w_qkv, w_o, w_up, w_down, w_out, ada_mods, alpha_coef, beta_coef):
        batch, tokens, ch = x_init.shape
        total = batch * tokens
        steps, heads, head_dim, dim = ada_mods.shape[0], w_o.shape[1], w_o.shape[2], w_o.shape[3]
        hidden = w_up.shape[2]
        micro, tm = total // GROUP, GROUP
        dims = (steps, stages, heads, head_dim, dim, micro, tm)
        any_spec = pl.BlockSpec(memory_space=pl.ANY)
        vmem_spec = pl.BlockSpec(memory_space=pltpu.VMEM)
        smem_spec = pl.BlockSpec(memory_space=pltpu.SMEM)
        x_out, h_last = pl.pallas_call(
            functools.partial(kernel, dims),
            out_shape=(pltpu.VMEM((micro, ch, tm), F32), pltpu.VMEM((total, dim), BF16)),
            in_specs=[any_spec] * 9 + [smem_spec, smem_spec],
            out_specs=(vmem_spec, vmem_spec),
            scratch_shapes=[
                pltpu.VMEM((ch, dim), BF16), pltpu.VMEM((steps * 6 * dim // TILE, TILE), F32),
                pltpu.VMEM((ch, dim), BF16), pltpu.VMEM((dim, 3 * dim), BF16), pltpu.VMEM((dim, dim), BF16),
                pltpu.VMEM((dim, hidden), BF16), pltpu.VMEM((hidden, dim), BF16),
                pltpu.VMEM((total, dim), BF16), pltpu.VMEM((total, ch), F32),
                pltpu.VMEM((dim, ch), BF16), pltpu.VMEM((3 * dim, dim), BF16), pltpu.VMEM((dim, dim), BF16),
                pltpu.VMEM((hidden, dim), BF16), pltpu.VMEM((dim, hidden), BF16),
                pltpu.VMEM((steps, 6, dim, TILE), F32),
                pltpu.VMEM((dim, tm), F32), pltpu.VMEM((dim, tm), F32), pltpu.VMEM((dim, tm), F32), pltpu.VMEM((dim, tm), F32),
                pltpu.VMEM((dim, tm), BF16), pltpu.VMEM((dim, tm), BF16),
                pltpu.VMEM((dim, tm), BF16), pltpu.VMEM((dim, tm), BF16), pltpu.VMEM((dim, tm), BF16),
                pltpu.VMEM((dim, tm), BF16), pltpu.VMEM((hidden, tm), BF16),
                pltpu.VMEM((steps, micro, dim, tm), BF16), pltpu.VMEM((steps, micro, ch, tm), BF16),
                pltpu.VMEM((steps, micro, dim, tm), BF16), pltpu.VMEM((steps, micro, ch, tm), BF16), pltpu.VMEM((micro, ch, tm), F32),
                pltpu.SemaphoreType.DMA((9,)),
                pltpu.SemaphoreType.DMA, pltpu.SemaphoreType.DMA((steps - 1, micro)),
                pltpu.SemaphoreType.DMA((stages,)), pltpu.SemaphoreType.DMA((steps - 1, micro)),
                pltpu.SemaphoreType.DMA((stages,)), pltpu.SemaphoreType.DMA,
            ],
            compiler_params=pltpu.CompilerParams(collective_id=0, has_side_effects=True, vmem_limit_bytes=60 * 1024 * 1024),
        )(x_init.reshape(total, ch), h_warm.reshape(stages - 1, total, dim), w_lat.reshape(ch, dim),
          w_qkv.reshape(dim, 3 * dim), w_o.reshape(heads * head_dim, dim), w_up.reshape(dim, hidden),
          w_down.reshape(hidden, dim), w_out.T, ada_mods.reshape(steps * 6 * dim // TILE, TILE), alpha_coef, beta_coef)
        x_out = x_out.transpose(0, 2, 1)
        return x_out.reshape(batch, tokens, ch), h_last.reshape(1, batch, tokens, dim)

    return jax.shard_map(stage_program, mesh=mesh,
                         in_specs=(P('data'), P(None, 'data'), P('stage'), P('stage'), P('stage'), P('stage'), P('stage'), P(), P(None, 'stage'), P(), P()),
                         out_specs=(P('data'), P('stage', 'data')), check_vma=False)
```

```python
import functools
import math

import jax
import jax.numpy as jnp
from jax import lax
from jax.experimental import pallas as pl
from jax.experimental.pallas import tpu as pltpu
from jax.sharding import PartitionSpec as P

MESH = pl.DeviceIdType.MESH
F32, BF16 = jnp.float32, jnp.bfloat16
GROUP = 256
TILE = 128
GELU_A = math.sqrt(2.0 / math.pi)
GELU_B = 0.044715


def dot(lhs, rhs):
    return lax.dot_general(lhs, rhs, (((1,), (0,)), ((), ())), preferred_element_type=F32)


def layer_norm(src, dst, mid, scale, shift):
    dim, tm = src.shape
    chunks = [slice(i, i + 64) for i in range(0, dim, 64)]

    def total(terms):
        part = sum(jnp.sum(term.reshape(8, 8, tm), axis=0) for term in terms)
        return jnp.sum(part, axis=0, keepdims=True) * (1.0 / dim)

    mean = total(src[rows, :] for rows in chunks)
    def squares():
        for rows in chunks:
            centered = src[rows, :] - mean
            mid[rows, :] = centered
            yield centered * centered
    var = total(squares())
    inv = lax.rsqrt(var + 1e-6)
    for rows in chunks:
        for lane in range(0, tm, TILE):
            tile = slice(lane, lane + TILE)
            dst[rows, tile] = (mid[rows, tile] * inv[:, tile] * scale[rows, :] + shift[rows, :]).astype(BF16)


def kernel(dims, x_hbm, warm_hbm, wlat_hbm, wqkv_hbm, wo_hbm, wup_hbm, wdown_hbm, wout_hbm, mods_hbm, alpha_ref, beta_ref,
           xo_ref, hl_ref,
           wout_ref, mods_ref, wlat_raw, wqkv_raw, wo_raw, wup_raw, wdown_raw, warm_raw, x_raw,
           wlat_t, wqkv_t, wo_t, wup_t, wdown_t, modb,
           mid_ref, mid2_ref, h_ref, hb_ref, h2_ref, h2b_ref, u_ref, u2_ref, q_ref, k_ref, v_ref, att_ref, hid_ref,
           b_in, x_in, b_out, x_out, x_f32,
           load_sem, hs_sem, hr_sem, xs_sem, xr_sem, fs_sem, fr_sem):
    steps, stages, heads, head_dim, dim, micro, tm = dims
    stage = lax.axis_index('stage')
    last = stages - 1
    hidden = wup_t.shape[0]
    slots = steps * micro
    others = (5, 3, 1, 4, 2, 0, 6)

    loads = [pltpu.make_async_copy(src, dst, load_sem.at[i]) for i, (src, dst) in enumerate((
        (x_hbm, x_raw), (wlat_hbm, wlat_raw), (wqkv_hbm, wqkv_raw), (wo_hbm, wo_raw),
        (wup_hbm, wup_raw), (wdown_hbm, wdown_raw), (wout_hbm, wout_ref)))]
    mods = pltpu.make_async_copy(mods_hbm, mods_ref, load_sem.at[8])
    warm = pltpu.make_async_copy(warm_hbm.at[jnp.maximum(stage - 1, 0)], warm_raw, load_sem.at[7])
    mods.start()
    loads[0].start()
    warm.start()
    for copy in loads[1:]:
        copy.start()

    barrier = pltpu.get_barrier_semaphore()
    for shift in range(1, stages):
        pl.semaphore_signal(barrier, inc=1, device_id={'stage': lax.rem(stage + shift, stages)}, device_id_type=MESH)

    def make_mods(t):
        for i in range(6):
            for c in range(dim // TILE):
                row = mods_ref[pl.ds((t * 6 + i) * (dim // TILE) + c, 1), :]
                if i in (1, 4):
                    row = row + 1.0
                modb[t, i, c * TILE:(c + 1) * TILE, :] = jnp.broadcast_to(row, (TILE, TILE)).T

    def make_inputs(m):
        xt = x_raw[m * tm:(m + 1) * tm, :].T
        x_f32[m] = xt
        x_in[0, m] = xt.astype(BF16)
        b_in[0, m] = warm_raw[m * tm:(m + 1) * tm, :].T

    mods.wait()
    make_mods(0)
    loads[0].wait()
    warm.wait()

    @pl.when(stage == 0)
    def _():
        warm_raw[...] = jnp.zeros_like(warm_raw)
    for copy in loads[1:]:
        copy.wait()
    make_inputs(0)
    wlat_t[...] = wlat_raw[...].T
    wqkv_t[...] = wqkv_raw[...].T

    def late_weights():
        wo_t[...] = wo_raw[...].T
        for j in range(hidden // dim):
            wup_t[j * dim:(j + 1) * dim, :] = wup_raw[:, j * dim:(j + 1) * dim].T * jnp.asarray(0.5, BF16)
            wdown_t[:, j * dim:(j + 1) * dim] = wdown_raw[j * dim:(j + 1) * dim, :].T
        for m in range(1, micro):
            make_inputs(m)

    def late_mods():
        for t in range(1, steps):
            make_mods(t)

    def h_copy(t, m):
        return pltpu.make_async_remote_copy(
            src_ref=b_out.at[t, m], dst_ref=b_in.at[t + 1, m], send_sem=hs_sem, recv_sem=hr_sem.at[t, m],
            device_id={'stage': jnp.minimum(stage + 1, last)}, device_id_type=MESH)

    def x_copy(t, m, dev):
        return pltpu.make_async_remote_copy(
            src_ref=x_out.at[t, m], dst_ref=x_in.at[t + 1, m], send_sem=xs_sem.at[dev], recv_sem=xr_sem.at[t, m],
            device_id={'stage': dev}, device_id_type=MESH)

    def f_copy(m, src, dev):
        return pltpu.make_async_remote_copy(
            src_ref=src.at[m], dst_ref=xo_ref.at[m], send_sem=fs_sem.at[dev], recv_sem=fr_sem,
            device_id={'stage': dev}, device_id_type=MESH)

    low_half = lax.rem(lax.broadcasted_iota(jnp.int32, (head_dim, 2 * TILE), 1), TILE) < head_dim
    score_scale = head_dim ** -0.5 * math.log2(math.e)
    tiles = [slice(i * TILE, (i + 1) * TILE) for i in range(tm // TILE)]
    halves = [slice(0, dim // 2), slice(dim // 2, dim)]
    zero_q = jnp.zeros((head_dim, TILE), BF16)
    zero_p = jnp.zeros((TILE, TILE), BF16)

    def step_of(slot):
        return lax.div(slot, micro), lax.rem(slot, micro)

    def attn_in(slot):
        t, m = step_of(slot)
        for rows in halves:
            h_ref[rows, :] = b_in[jnp.where(stage > 0, t, 0), m, rows, :].astype(F32) + dot(wlat_t[rows, :], x_in[t, m])

    def attn_norm(slot):
        t, _ = step_of(slot)
        layer_norm(h_ref, u_ref, mid_ref, modb.at[t, 1], modb.at[t, 0])

    def project(part, dst):
        for rows in halves:
            dst[rows, :] = dot(wqkv_t[part * dim + rows.start:part * dim + rows.stop, :], u_ref[...]).astype(BF16)

    def score_dots():
        scores = []
        for hp in range(heads // 2):
            rows = slice(hp * TILE, (hp + 1) * TILE)
            q_pair = q_ref[rows, :]
            k_pair = k_ref[rows, :].T
            for span in tiles:
                q_blk = jnp.concatenate([
                    jnp.concatenate([q_pair[:head_dim, span], zero_q], axis=1),
                    jnp.concatenate([zero_q, q_pair[head_dim:, span]], axis=1)], axis=0)
                full = dot(k_pair[span, :], q_blk)
                scores.append(jnp.where(low_half, full[:head_dim], full[head_dim:]))
        return scores

    def softmax(scores):
        top = jnp.max(scores, axis=0, keepdims=True)
        expd = jnp.exp2((scores - top) * score_scale)
        prob = (expd * (1.0 / jnp.sum(expd, axis=0, keepdims=True))).astype(BF16)
        nought = jnp.zeros_like(prob)
        return jnp.concatenate([jnp.where(low_half, prob, nought), jnp.where(low_half, nought, prob)], axis=0)

    def value_dots(probs):
        for head in range(heads):
            hp, span = head // 2, tiles[head % 2]
            p_blk = jnp.concatenate([
                jnp.concatenate([probs[2 * hp][:, span], zero_p], axis=1),
                jnp.concatenate([zero_p, probs[2 * hp + 1][:, span]], axis=1)], axis=0)
            rows = slice(head * head_dim, (head + 1) * head_dim)
            att_ref[rows, :] = dot(v_ref[rows, :], p_blk).astype(BF16)

    def attn_out(slot):
        t, _ = step_of(slot)
        for rows in halves:
            proj = dot(wo_t[rows, :], att_ref[...])
            for tile in tiles:
                h2_ref[rows, tile] = hb_ref[rows, tile] + modb[t, 2, rows, :] * proj[:, tile]

    def mlp_norm(slot):
        t, _ = step_of(slot)
        layer_norm(h2_ref, u2_ref, mid2_ref, modb.at[t, 4], modb.at[t, 3])

    def mlp_up(j):
        rows = slice(j * GROUP, (j + 1) * GROUP)
        half = dot(wup_t[rows, :], u2_ref[...])
        inner = half * (half * half * (8.0 * GELU_A * GELU_B) + 2.0 * GELU_A)
        hid_ref[rows, :] = (half + half * jnp.tanh(inner)).astype(BF16)

    def mlp_down(slot):
        t, m = step_of(slot)
        for rows in halves:
            down = dot(wdown_t[rows, :], hid_ref[...])
            for tile in tiles:
                b_out[t, m, rows, tile] = (h2b_ref[rows, tile] + modb[t, 5, rows, :] * down[:, tile]).astype(BF16)

    def latent(slot):
        t, m = step_of(slot)
        eps = dot(wout_ref[...], b_out[t, m])
        x_next = alpha_ref[t] * x_f32[m] + beta_ref[t] * eps
        x_f32[m] = x_next
        x_out[t, m] = x_next.astype(BF16)
        hl_ref[pl.ds(m * tm, tm), :] = b_out[t, m].T

    def receive(slot):
        t, m = step_of(slot)

        @pl.when(jnp.logical_and(t > 0, stage > 0))
        def _():
            h_copy(t - 1, m).wait_recv()

        @pl.when(jnp.logical_and(t > 0, stage < last))
        def _():
            x_copy(t - 1, m, 0).wait_recv()

    def send_stage(slot):
        t, m = step_of(slot)

        @pl.when(jnp.logical_and(t < steps - 1, stage < last))
        def _():
            h_copy(t, m).start()

    def send_latent(slot):
        t, m = step_of(slot)

        @pl.when(jnp.logical_and(t < steps - 1, stage == last))
        def _():
            x_in[t + 1, m] = x_out[t, m]
            for dev in others:
                x_copy(t, m, dev).start()

        @pl.when(jnp.logical_and(t == steps - 1, stage == last))
        def _():
            xo_ref[m] = x_f32[m]
            for dev in (1, 3, 5, 6):
                f_copy(m, x_f32, dev).start()

    def block(attn=None, out=None, mlp=None, lat=None, extra=None):
        ups = hidden // GROUP
        if mlp is not None:
            h2b_ref[...] = h2_ref[...]
        if out is not None:
            hb_ref[...] = h_ref[...]
        if attn is not None:
            attn_in(attn)
        if lat is not None:
            latent(lat)
        if mlp is not None:
            for j in range(4):
                mlp_up(j)
        if attn is not None:
            attn_norm(attn)
            project(0, q_ref)
            project(1, k_ref)
        if mlp is not None:
            for j in range(4, ups):
                mlp_up(j)
        if attn is not None:
            scores = score_dots()
            project(2, v_ref)
        if out is not None:
            attn_out(out)
            mlp_norm(out)
        if extra is not None:
            extra()
        if attn is not None:
            value_dots([softmax(s) for s in scores])
        if mlp is not None:
            mlp_down(mlp)
            send_stage(mlp)
        if lat is not None:
            send_latent(lat)

    block(attn=0, extra=late_weights)
    block(attn=1, out=0, extra=late_mods)
    pl.semaphore_wait(barrier, stages - 1)

    def slot_body(slot, carry):
        t, m = step_of(slot)
        receive(slot)
        block(slot, slot - 1, slot - 2, slot - 3)
        return carry
    block(2, 1, 0)
    lax.fori_loop(3, slots, slot_body, 0)
    block(None, slots - 1, slots - 2, slots - 3)
    block(None, None, slots - 1, slots - 2)
    block(None, None, None, slots - 1)

    def whole(src, dst, sem, dev):
        return pltpu.make_async_remote_copy(
            src_ref=src, dst_ref=dst, send_sem=sem, recv_sem=fr_sem, device_id={'stage': dev}, device_id_type=MESH)

    sent = pl.ds(0, steps - 1)

    @pl.when(stage < last)
    def _():
        whole(xo_ref, xo_ref, fs_sem.at[0], 0).wait_recv()
    for src, dev in ((5, 4), (3, 2), (1, 0)):
        @pl.when(stage == src)
        def _(dev=dev):
            whole(xo_ref, xo_ref, fs_sem.at[dev], dev).start()

    @pl.when(stage < last)
    def _():
        whole(b_out.at[sent], b_in.at[pl.ds(1, steps - 1)], hs_sem, jnp.minimum(stage + 1, last)).wait_send()
    for src, dev in ((5, 4), (3, 2), (1, 0)):
        @pl.when(stage == src)
        def _(dev=dev):
            whole(xo_ref, xo_ref, fs_sem.at[dev], dev).wait_send()

    @pl.when(stage == last)
    def _():
        for dev in others:
            whole(x_out.at[sent], x_in.at[pl.ds(1, steps - 1)], xs_sem.at[dev], dev).wait_send()
        for dev in (5, 3, 1, 6):
            whole(x_f32, xo_ref, fs_sem.at[dev], dev).wait_send()


def solution(mesh):
    stages = mesh.shape['stage']

    def stage_program(x_init, h_warm, w_lat, w_qkv, w_o, w_up, w_down, w_out, ada_mods, alpha_coef, beta_coef):
        batch, tokens, ch = x_init.shape
        total = batch * tokens
        steps, heads, head_dim, dim = ada_mods.shape[0], w_o.shape[1], w_o.shape[2], w_o.shape[3]
        hidden = w_up.shape[2]
        micro, tm = total // GROUP, GROUP
        dims = (steps, stages, heads, head_dim, dim, micro, tm)
        any_spec = pl.BlockSpec(memory_space=pl.ANY)
        vmem_spec = pl.BlockSpec(memory_space=pltpu.VMEM)
        smem_spec = pl.BlockSpec(memory_space=pltpu.SMEM)
        x_out, h_last = pl.pallas_call(
            functools.partial(kernel, dims),
            out_shape=(pltpu.VMEM((micro, ch, tm), F32), pltpu.VMEM((total, dim), BF16)),
            in_specs=[any_spec] * 9 + [smem_spec, smem_spec],
            out_specs=(vmem_spec, vmem_spec),
            scratch_shapes=[
                pltpu.VMEM((ch, dim), BF16), pltpu.VMEM((steps * 6 * dim // TILE, TILE), F32),
                pltpu.VMEM((ch, dim), BF16), pltpu.VMEM((dim, 3 * dim), BF16), pltpu.VMEM((dim, dim), BF16),
                pltpu.VMEM((dim, hidden), BF16), pltpu.VMEM((hidden, dim), BF16),
                pltpu.VMEM((total, dim), BF16), pltpu.VMEM((total, ch), F32),
                pltpu.VMEM((dim, ch), BF16), pltpu.VMEM((3 * dim, dim), BF16), pltpu.VMEM((dim, dim), BF16),
                pltpu.VMEM((hidden, dim), BF16), pltpu.VMEM((dim, hidden), BF16),
                pltpu.VMEM((steps, 6, dim, TILE), F32),
                pltpu.VMEM((dim, tm), F32), pltpu.VMEM((dim, tm), F32), pltpu.VMEM((dim, tm), F32), pltpu.VMEM((dim, tm), F32), pltpu.VMEM((dim, tm), F32), pltpu.VMEM((dim, tm), F32),
                pltpu.VMEM((dim, tm), BF16), pltpu.VMEM((dim, tm), BF16),
                pltpu.VMEM((dim, tm), BF16), pltpu.VMEM((dim, tm), BF16), pltpu.VMEM((dim, tm), BF16),
                pltpu.VMEM((dim, tm), BF16), pltpu.VMEM((hidden, tm), BF16),
                pltpu.VMEM((steps, micro, dim, tm), BF16), pltpu.VMEM((steps, micro, ch, tm), BF16),
                pltpu.VMEM((steps, micro, dim, tm), BF16), pltpu.VMEM((steps, micro, ch, tm), BF16), pltpu.VMEM((micro, ch, tm), F32),
                pltpu.SemaphoreType.DMA((9,)),
                pltpu.SemaphoreType.DMA, pltpu.SemaphoreType.DMA((steps - 1, micro)),
                pltpu.SemaphoreType.DMA((stages,)), pltpu.SemaphoreType.DMA((steps - 1, micro)),
                pltpu.SemaphoreType.DMA((stages,)), pltpu.SemaphoreType.DMA,
            ],
            compiler_params=pltpu.CompilerParams(collective_id=0, has_side_effects=True, vmem_limit_bytes=60 * 1024 * 1024),
        )(x_init.reshape(total, ch), h_warm.reshape(stages - 1, total, dim), w_lat.reshape(ch, dim),
          w_qkv.reshape(dim, 3 * dim), w_o.reshape(heads * head_dim, dim), w_up.reshape(dim, hidden),
          w_down.reshape(hidden, dim), w_out.T, ada_mods.reshape(steps * 6 * dim // TILE, TILE), alpha_coef, beta_coef)
        x_out = x_out.transpose(0, 2, 1)
        return x_out.reshape(batch, tokens, ch), h_last.reshape(1, batch, tokens, dim)

    return jax.shard_map(stage_program, mesh=mesh,
                         in_specs=(P('data'), P(None, 'data'), P('stage'), P('stage'), P('stage'), P('stage'), P('stage'), P(), P(None, 'stage'), P(), P()),
                         out_specs=(P('data'), P('stage', 'data')), check_vma=False)
```

```python
import functools
import math

import jax
import jax.numpy as jnp
from jax import lax
from jax.experimental import pallas as pl
from jax.experimental.pallas import tpu as pltpu
from jax.sharding import PartitionSpec as P

MESH = pl.DeviceIdType.MESH
F32, BF16 = jnp.float32, jnp.bfloat16
GROUP = 256
TILE = 128
GELU_A = math.sqrt(2.0 / math.pi)
GELU_B = 0.044715


def dot(lhs, rhs):
    return lax.dot_general(lhs, rhs, (((1,), (0,)), ((), ())), preferred_element_type=F32)


def layer_norm(src, dst, mid, scale, shift):
    dim, tm = src.shape
    chunks = [slice(i, i + 64) for i in range(0, dim, 64)]

    def total(terms):
        part = sum(jnp.sum(term.reshape(8, 8, tm), axis=0) for term in terms)
        return jnp.sum(part, axis=0, keepdims=True) * (1.0 / dim)

    mean = total(src[rows, :] for rows in chunks)
    def squares():
        for rows in chunks:
            centered = src[rows, :] - mean
            mid[rows, :] = centered
            yield centered * centered
    var = total(squares())
    inv = lax.rsqrt(var + 1e-6)
    for rows in chunks:
        for lane in range(0, tm, TILE):
            tile = slice(lane, lane + TILE)
            dst[rows, tile] = (mid[rows, tile] * inv[:, tile] * scale[rows, :] + shift[rows, :]).astype(BF16)


def kernel(dims, x_hbm, warm_hbm, wlat_hbm, wqkv_hbm, wo_hbm, wup_hbm, wdown_hbm, wout_hbm, mods_hbm, alpha_ref, beta_ref,
           xo_ref, hl_ref,
           wout_ref, mods_ref, wlat_raw, wqkv_raw, wo_raw, wup_raw, wdown_raw, warm_raw, x_raw,
           wlat_t, wqkv_t, wo_t, wup_t, wdown_t, modb,
           mid_ref, mid2_ref, h_ring, h2_ring, u_ref, u2_ref, q_ref, k_ref, v_ref, att_ref, hid_ref,
           b_in, x_in, b_out, x_out, x_f32,
           load_sem, hs_sem, hr_sem, xs_sem, xr_sem, fs_sem, fr_sem, rs_sem):
    steps, stages, heads, head_dim, dim, micro, tm = dims
    stage = lax.axis_index('stage')
    last = stages - 1
    hidden = wup_t.shape[0]
    slots = steps * micro
    others = (5, 3, 1, 4, 2, 0, 6)

    loads = [pltpu.make_async_copy(src, dst, load_sem.at[i]) for i, (src, dst) in enumerate((
        (x_hbm, x_raw), (wlat_hbm, wlat_raw), (wqkv_hbm, wqkv_raw), (wo_hbm, wo_raw),
        (wup_hbm, wup_raw), (wdown_hbm, wdown_raw), (wout_hbm, wout_ref)))]
    mods = pltpu.make_async_copy(mods_hbm, mods_ref, load_sem.at[8])
    warm = pltpu.make_async_copy(warm_hbm.at[jnp.maximum(stage - 1, 0)], warm_raw, load_sem.at[7])
    mods.start()
    loads[0].start()
    warm.start()
    for copy in loads[1:]:
        copy.start()

    barrier = pltpu.get_barrier_semaphore()
    for shift in range(1, stages):
        pl.semaphore_signal(barrier, inc=1, device_id={'stage': lax.rem(stage + shift, stages)}, device_id_type=MESH)

    def make_mods(t):
        for i in range(6):
            for c in range(dim // TILE):
                row = mods_ref[pl.ds((t * 6 + i) * (dim // TILE) + c, 1), :]
                if i in (1, 4):
                    row = row + 1.0
                modb[t, i, c * TILE:(c + 1) * TILE, :] = jnp.broadcast_to(row, (TILE, TILE)).T

    def make_inputs(m):
        xt = x_raw[m * tm:(m + 1) * tm, :].T
        x_f32[m] = xt
        x_in[0, m] = xt.astype(BF16)
        b_in[0, m] = warm_raw[m * tm:(m + 1) * tm, :].T

    mods.wait()
    make_mods(0)
    loads[0].wait()
    warm.wait()

    @pl.when(stage == 0)
    def _():
        warm_raw[...] = jnp.zeros_like(warm_raw)
    for copy in loads[1:]:
        copy.wait()
    make_inputs(0)
    wlat_t[...] = wlat_raw[...].T
    wqkv_t[...] = wqkv_raw[...].T

    def late_weights():
        wo_t[...] = wo_raw[...].T
        for j in range(hidden // dim):
            wup_t[j * dim:(j + 1) * dim, :] = wup_raw[:, j * dim:(j + 1) * dim].T * jnp.asarray(0.5, BF16)
            wdown_t[:, j * dim:(j + 1) * dim] = wdown_raw[j * dim:(j + 1) * dim, :].T
        for m in range(1, micro):
            make_inputs(m)

    def late_mods():
        for t in range(1, steps):
            make_mods(t)

    def h_copy(t, m):
        return pltpu.make_async_remote_copy(
            src_ref=b_out.at[t, m], dst_ref=b_in.at[t + 1, m], send_sem=hs_sem, recv_sem=hr_sem.at[t, m],
            device_id={'stage': jnp.minimum(stage + 1, last)}, device_id_type=MESH)

    def x_copy(t, m, dev):
        return pltpu.make_async_remote_copy(
            src_ref=x_out.at[t, m], dst_ref=x_in.at[t + 1, m], send_sem=xs_sem.at[dev], recv_sem=xr_sem.at[t, m],
            device_id={'stage': dev}, device_id_type=MESH)

    def f_copy(m, src, dev):
        return pltpu.make_async_remote_copy(
            src_ref=src.at[m], dst_ref=xo_ref.at[m], send_sem=fs_sem.at[dev], recv_sem=fr_sem.at[lax.div(m, micro - 1)],
            device_id={'stage': dev}, device_id_type=MESH)

    low_half = lax.rem(lax.broadcasted_iota(jnp.int32, (head_dim, 2 * TILE), 1), TILE) < head_dim
    score_scale = head_dim ** -0.5 * math.log2(math.e)
    tiles = [slice(i * TILE, (i + 1) * TILE) for i in range(tm // TILE)]
    halves = [slice(0, dim // 2), slice(dim // 2, dim)]
    zero_q = jnp.zeros((head_dim, TILE), BF16)
    zero_p = jnp.zeros((TILE, TILE), BF16)

    def step_of(slot):
        return lax.div(slot, micro), lax.rem(slot, micro)

    def attn_in(slot):
        t, m = step_of(slot)
        for rows in halves:
            h_ring[lax.rem(slot, 2), rows, :] = b_in[jnp.where(stage > 0, t, 0), m, rows, :].astype(F32) + dot(wlat_t[rows, :], x_in[t, m])

    def attn_norm(slot):
        t, _ = step_of(slot)
        layer_norm(h_ring.at[lax.rem(slot, 2)], u_ref, mid_ref, modb.at[t, 1], modb.at[t, 0])

    def project(part, dst):
        for rows in halves:
            dst[rows, :] = dot(wqkv_t[part * dim + rows.start:part * dim + rows.stop, :], u_ref[...]).astype(BF16)

    def score_dots():
        scores = []
        for hp in range(heads // 2):
            rows = slice(hp * TILE, (hp + 1) * TILE)
            q_pair = q_ref[rows, :]
            k_pair = k_ref[rows, :].T
            for span in tiles:
                q_blk = jnp.concatenate([
                    jnp.concatenate([q_pair[:head_dim, span], zero_q], axis=1),
                    jnp.concatenate([zero_q, q_pair[head_dim:, span]], axis=1)], axis=0)
                full = dot(k_pair[span, :], q_blk)
                scores.append(jnp.where(low_half, full[:head_dim], full[head_dim:]))
        return scores

    def softmax(scores):
        top = jnp.max(scores, axis=0, keepdims=True)
        expd = jnp.exp2((scores - top) * score_scale)
        prob = (expd * (1.0 / jnp.sum(expd, axis=0, keepdims=True))).astype(BF16)
        nought = jnp.zeros_like(prob)
        return jnp.concatenate([jnp.where(low_half, prob, nought), jnp.where(low_half, nought, prob)], axis=0)

    def value_dots(probs):
        for head in range(heads):
            hp, span = head // 2, tiles[head % 2]
            p_blk = jnp.concatenate([
                jnp.concatenate([probs[2 * hp][:, span], zero_p], axis=1),
                jnp.concatenate([zero_p, probs[2 * hp + 1][:, span]], axis=1)], axis=0)
            rows = slice(head * head_dim, (head + 1) * head_dim)
            att_ref[rows, :] = dot(v_ref[rows, :], p_blk).astype(BF16)

    def attn_out(slot):
        t, _ = step_of(slot)
        for rows in halves:
            proj = dot(wo_t[rows, :], att_ref[...])
            for tile in tiles:
                h2_ring[lax.rem(slot, 2), rows, tile] = h_ring[lax.rem(slot, 2), rows, tile] + modb[t, 2, rows, :] * proj[:, tile]

    def mlp_norm(slot):
        t, _ = step_of(slot)
        layer_norm(h2_ring.at[lax.rem(slot, 2)], u2_ref, mid2_ref, modb.at[t, 4], modb.at[t, 3])

    def mlp_up(j):
        rows = slice(j * GROUP, (j + 1) * GROUP)
        half = dot(wup_t[rows, :], u2_ref[...])
        inner = half * (half * half * (8.0 * GELU_A * GELU_B) + 2.0 * GELU_A)
        hid_ref[rows, :] = (half + half * jnp.tanh(inner)).astype(BF16)

    def mlp_down(slot):
        t, m = step_of(slot)
        for rows in halves:
            down = dot(wdown_t[rows, :], hid_ref[...])
            for tile in tiles:
                b_out[t, m, rows, tile] = (h2_ring[lax.rem(slot, 2), rows, tile] + modb[t, 5, rows, :] * down[:, tile]).astype(BF16)

    def latent(slot):
        t, m = step_of(slot)
        eps = dot(wout_ref[...], b_out[t, m])
        x_next = alpha_ref[t] * x_f32[m] + beta_ref[t] * eps
        x_f32[m] = x_next
        x_out[t, m] = x_next.astype(BF16)
        hl_ref[pl.ds(m * tm, tm), :] = b_out[t, m].T

    def receive(slot):
        t, m = step_of(slot)

        @pl.when(jnp.logical_and(t > 0, stage > 0))
        def _():
            h_copy(t - 1, m).wait_recv()

        @pl.when(jnp.logical_and(t > 0, stage < last))
        def _():
            x_copy(t - 1, m, 0).wait_recv()

    def send_stage(slot):
        t, m = step_of(slot)

        @pl.when(jnp.logical_and(t < steps - 1, stage < last))
        def _():
            h_copy(t, m).start()

    def send_latent(slot):
        t, m = step_of(slot)

        @pl.when(jnp.logical_and(t < steps - 1, stage == last))
        def _():
            x_in[t + 1, m] = x_out[t, m]
            for dev in others:
                x_copy(t, m, dev).start()

        @pl.when(jnp.logical_and(t == steps - 1, stage == last))
        def _():
            xo_ref[m] = x_f32[m]
            @pl.when(m == micro - 1)
            def _():
                f_copy(m, x_f32, 0).start()
            for dev in (1, 3, 5, 6):
                f_copy(m, x_f32, dev).start()

    def block(attn=None, out=None, mlp=None, lat=None, extra=None):
        ups = hidden // GROUP
        if attn is not None:
            attn_in(attn)
        if lat is not None:
            latent(lat)
        if mlp is not None:
            for j in range(4):
                mlp_up(j)
        if attn is not None:
            attn_norm(attn)
            project(0, q_ref)
            project(1, k_ref)
        if mlp is not None:
            for j in range(4, ups):
                mlp_up(j)
        if attn is not None:
            scores = score_dots()
            project(2, v_ref)
        if out is not None:
            attn_out(out)
            mlp_norm(out)
        if extra is not None:
            extra()
        if attn is not None:
            value_dots([softmax(s) for s in scores])
        if mlp is not None:
            mlp_down(mlp)
            send_stage(mlp)
        if lat is not None:
            send_latent(lat)

    block(attn=0, extra=late_weights)
    block(attn=1, out=0, extra=late_mods)
    pl.semaphore_wait(barrier, stages - 1)

    def slot_body(slot, carry):
        t, m = step_of(slot)
        receive(slot)
        block(slot, slot - 1, slot - 2, slot - 3)
        return carry
    block(2, 1, 0)
    lax.fori_loop(3, slots, slot_body, 0)
    block(None, slots - 1, slots - 2, slots - 3)
    block(None, None, slots - 1, slots - 2)
    block(None, None, None, slots - 1)

    def whole(src, dst, sem, dev):
        return pltpu.make_async_remote_copy(
            src_ref=src, dst_ref=dst, send_sem=sem, recv_sem=fr_sem.at[0], device_id={'stage': dev}, device_id_type=MESH)

    def relay(part, dev):
        span = pl.ds(0, micro - 1) if part == 0 else pl.ds(micro - 1, 1)
        return pltpu.make_async_remote_copy(
            src_ref=xo_ref.at[span], dst_ref=xo_ref.at[span], send_sem=rs_sem.at[part], recv_sem=fr_sem.at[part],
            device_id={'stage': dev}, device_id_type=MESH)

    sent = pl.ds(0, steps - 1)
    for part in range(2):
        @pl.when(stage < last)
        def _(part=part):
            relay(part, 0).wait_recv()
        for src, dev in ((5, 4), (3, 2), (1, 0)):
            if part == 0 or dev > 0:
                @pl.when(stage == src)
                def _(part=part, dev=dev):
                    relay(part, dev).start()

    @pl.when(stage < last)
    def _():
        whole(b_out.at[sent], b_in.at[pl.ds(1, steps - 1)], hs_sem, jnp.minimum(stage + 1, last)).wait_send()
    for src, dev in ((5, 4), (3, 2), (1, 0)):
        for part in range(2):
            if part == 0 or dev > 0:
                @pl.when(stage == src)
                def _(part=part, dev=dev):
                    relay(part, dev).wait_send()

    @pl.when(stage == last)
    def _():
        for dev in others:
            whole(x_out.at[sent], x_in.at[pl.ds(1, steps - 1)], xs_sem.at[dev], dev).wait_send()
        for dev in (1, 3, 5, 6):
            whole(x_f32, xo_ref, fs_sem.at[dev], dev).wait_send()
        f_copy(micro - 1, x_f32, 0).wait_send()


def solution(mesh):
    stages = mesh.shape['stage']

    def stage_program(x_init, h_warm, w_lat, w_qkv, w_o, w_up, w_down, w_out, ada_mods, alpha_coef, beta_coef):
        batch, tokens, ch = x_init.shape
        total = batch * tokens
        steps, heads, head_dim, dim = ada_mods.shape[0], w_o.shape[1], w_o.shape[2], w_o.shape[3]
        hidden = w_up.shape[2]
        micro, tm = total // GROUP, GROUP
        dims = (steps, stages, heads, head_dim, dim, micro, tm)
        any_spec = pl.BlockSpec(memory_space=pl.ANY)
        vmem_spec = pl.BlockSpec(memory_space=pltpu.VMEM)
        smem_spec = pl.BlockSpec(memory_space=pltpu.SMEM)
        x_out, h_last = pl.pallas_call(
            functools.partial(kernel, dims),
            out_shape=(pltpu.VMEM((micro, ch, tm), F32), pltpu.VMEM((total, dim), BF16)),
            in_specs=[any_spec] * 9 + [smem_spec, smem_spec],
            out_specs=(vmem_spec, vmem_spec),
            scratch_shapes=[
                pltpu.VMEM((ch, dim), BF16), pltpu.VMEM((steps * 6 * dim // TILE, TILE), F32),
                pltpu.VMEM((ch, dim), BF16), pltpu.VMEM((dim, 3 * dim), BF16), pltpu.VMEM((dim, dim), BF16),
                pltpu.VMEM((dim, hidden), BF16), pltpu.VMEM((hidden, dim), BF16),
                pltpu.VMEM((total, dim), BF16), pltpu.VMEM((total, ch), F32),
                pltpu.VMEM((dim, ch), BF16), pltpu.VMEM((3 * dim, dim), BF16), pltpu.VMEM((dim, dim), BF16),
                pltpu.VMEM((hidden, dim), BF16), pltpu.VMEM((dim, hidden), BF16),
                pltpu.VMEM((steps, 6, dim, TILE), F32),
                pltpu.VMEM((dim, tm), F32), pltpu.VMEM((dim, tm), F32), pltpu.VMEM((2, dim, tm), F32), pltpu.VMEM((2, dim, tm), F32),
                pltpu.VMEM((dim, tm), BF16), pltpu.VMEM((dim, tm), BF16),
                pltpu.VMEM((dim, tm), BF16), pltpu.VMEM((dim, tm), BF16), pltpu.VMEM((dim, tm), BF16),
                pltpu.VMEM((dim, tm), BF16), pltpu.VMEM((hidden, tm), BF16),
                pltpu.VMEM((steps, micro, dim, tm), BF16), pltpu.VMEM((steps, micro, ch, tm), BF16),
                pltpu.VMEM((steps, micro, dim, tm), BF16), pltpu.VMEM((steps, micro, ch, tm), BF16), pltpu.VMEM((micro, ch, tm), F32),
                pltpu.SemaphoreType.DMA((9,)),
                pltpu.SemaphoreType.DMA, pltpu.SemaphoreType.DMA((steps - 1, micro)),
                pltpu.SemaphoreType.DMA((stages,)), pltpu.SemaphoreType.DMA((steps - 1, micro)),
                pltpu.SemaphoreType.DMA((stages,)), pltpu.SemaphoreType.DMA((2,)), pltpu.SemaphoreType.DMA((2,)),
            ],
            compiler_params=pltpu.CompilerParams(collective_id=0, has_side_effects=True, vmem_limit_bytes=60 * 1024 * 1024),
        )(x_init.reshape(total, ch), h_warm.reshape(stages - 1, total, dim), w_lat.reshape(ch, dim),
          w_qkv.reshape(dim, 3 * dim), w_o.reshape(heads * head_dim, dim), w_up.reshape(dim, hidden),
          w_down.reshape(hidden, dim), w_out.T, ada_mods.reshape(steps * 6 * dim // TILE, TILE), alpha_coef, beta_coef)
        x_out = x_out.transpose(0, 2, 1)
        return x_out.reshape(batch, tokens, ch), h_last.reshape(1, batch, tokens, dim)

    return jax.shard_map(stage_program, mesh=mesh,
                         in_specs=(P('data'), P(None, 'data'), P('stage'), P('stage'), P('stage'), P('stage'), P('stage'), P(), P(None, 'stage'), P(), P()),
                         out_specs=(P('data'), P('stage', 'data')), check_vma=False)
```

```python
import functools
import math

import jax
import jax.numpy as jnp
from jax import lax
from jax.experimental import pallas as pl
from jax.experimental.pallas import tpu as pltpu
from jax.sharding import PartitionSpec as P

MESH = pl.DeviceIdType.MESH
F32, BF16 = jnp.float32, jnp.bfloat16
GROUP = 256
TILE = 128
GELU_A = math.sqrt(2.0 / math.pi)
GELU_B = 0.044715


def dot(lhs, rhs):
    return lax.dot_general(lhs, rhs, (((1,), (0,)), ((), ())), preferred_element_type=F32)


def layer_norm(src, dst, mid, scale, shift):
    dim, tm = src.shape
    chunks = [slice(i, i + 64) for i in range(0, dim, 64)]

    def total(terms):
        part = sum(jnp.sum(term.reshape(8, 8, tm), axis=0) for term in terms)
        return jnp.sum(part, axis=0, keepdims=True) * (1.0 / dim)

    mean = total(src[rows, :] for rows in chunks)
    def squares():
        for rows in chunks:
            centered = src[rows, :] - mean
            mid[rows, :] = centered
            yield centered * centered
    var = total(squares())
    inv = lax.rsqrt(var + 1e-6)
    for rows in chunks:
        for lane in range(0, tm, TILE):
            tile = slice(lane, lane + TILE)
            dst[rows, tile] = (mid[rows, tile] * inv[:, tile] * scale[rows, :] + shift[rows, :]).astype(BF16)


def kernel(dims, x_hbm, warm_hbm, wlat_hbm, wqkv_hbm, wo_hbm, wup_hbm, wdown_hbm, wout_hbm, mods_hbm, alpha_ref, beta_ref,
           xo_ref, hl_ref,
           wout_ref, mods_ref, wlat_raw, wqkv_raw, wo_raw, wup_raw, wdown_raw, warm_raw, x_raw,
           wlat_t, wqkv_t, wo_t, wup_t, wdown_t, modb,
           mid_ref, mid2_ref, h_ring, h2_ring, u_ref, u2_ref, q_ref, k_ref, v_ref, att_ref, hid_ref,
           b_in, x_in, b_out, x_out, x_f32,
           load_sem, hs_sem, hr_sem, xs_sem, xr_sem, fs_sem, fr_sem, rs_sem):
    steps, stages, heads, head_dim, dim, micro, tm = dims
    stage = lax.axis_index('stage')
    last = stages - 1
    hidden = wup_t.shape[0]
    slots = steps * micro
    others = (5, 3, 1, 4, 2, 0, 6)

    loads = [pltpu.make_async_copy(src, dst, load_sem.at[i]) for i, (src, dst) in enumerate((
        (x_hbm, x_raw), (wlat_hbm, wlat_raw), (wqkv_hbm, wqkv_raw), (wo_hbm, wo_raw),
        (wup_hbm, wup_raw), (wdown_hbm, wdown_raw), (wout_hbm, wout_ref)))]
    mods = pltpu.make_async_copy(mods_hbm, mods_ref, load_sem.at[8])
    warm = pltpu.make_async_copy(warm_hbm.at[jnp.maximum(stage - 1, 0)], warm_raw, load_sem.at[7])
    mods.start()
    loads[0].start()
    warm.start()
    for copy in loads[1:]:
        copy.start()

    barrier = pltpu.get_barrier_semaphore()
    for shift in range(1, stages):
        pl.semaphore_signal(barrier, inc=1, device_id={'stage': lax.rem(stage + shift, stages)}, device_id_type=MESH)

    def make_mods(t):
        for i in range(6):
            for c in range(dim // TILE):
                row = mods_ref[pl.ds((t * 6 + i) * (dim // TILE) + c, 1), :]
                if i in (1, 4):
                    row = row + 1.0
                modb[t, i, c * TILE:(c + 1) * TILE, :] = jnp.broadcast_to(row, (TILE, TILE)).T

    def make_inputs(m):
        xt = x_raw[m * tm:(m + 1) * tm, :].T
        x_f32[m] = xt
        x_in[0, m] = xt.astype(BF16)
        b_in[0, m] = warm_raw[m * tm:(m + 1) * tm, :].T

    mods.wait()
    make_mods(0)
    loads[0].wait()
    warm.wait()

    @pl.when(stage == 0)
    def _():
        warm_raw[...] = jnp.zeros_like(warm_raw)
    for copy in loads[1:3]:
        copy.wait()
    make_inputs(0)
    wlat_t[...] = wlat_raw[...].T
    wqkv_t[...] = wqkv_raw[...].T
    for copy in loads[3:]:
        copy.wait()

    def late_weights():
        wo_t[...] = wo_raw[...].T
        for j in range(hidden // dim):
            wup_t[j * dim:(j + 1) * dim, :] = wup_raw[:, j * dim:(j + 1) * dim].T * jnp.asarray(0.5, BF16)
            wdown_t[:, j * dim:(j + 1) * dim] = wdown_raw[j * dim:(j + 1) * dim, :].T
        for m in range(1, micro):
            make_inputs(m)

    def late_mods():
        for t in range(1, steps):
            make_mods(t)

    def h_copy(t, m):
        return pltpu.make_async_remote_copy(
            src_ref=b_out.at[t, m], dst_ref=b_in.at[t + 1, m], send_sem=hs_sem, recv_sem=hr_sem.at[t, m],
            device_id={'stage': jnp.minimum(stage + 1, last)}, device_id_type=MESH)

    def x_copy(t, m, dev):
        return pltpu.make_async_remote_copy(
            src_ref=x_out.at[t, m], dst_ref=x_in.at[t + 1, m], send_sem=xs_sem.at[dev], recv_sem=xr_sem.at[t, m],
            device_id={'stage': dev}, device_id_type=MESH)

    def f_copy(m, src, dev):
        return pltpu.make_async_remote_copy(
            src_ref=src.at[m], dst_ref=xo_ref.at[m], send_sem=fs_sem.at[dev], recv_sem=fr_sem.at[lax.div(m, micro - 1)],
            device_id={'stage': dev}, device_id_type=MESH)

    low_half = lax.rem(lax.broadcasted_iota(jnp.int32, (head_dim, 2 * TILE), 1), TILE) < head_dim
    score_scale = head_dim ** -0.5 * math.log2(math.e)
    tiles = [slice(i * TILE, (i + 1) * TILE) for i in range(tm // TILE)]
    halves = [slice(0, dim // 2), slice(dim // 2, dim)]
    zero_q = jnp.zeros((head_dim, TILE), BF16)
    zero_p = jnp.zeros((TILE, TILE), BF16)

    def step_of(slot):
        return lax.div(slot, micro), lax.rem(slot, micro)

    def attn_in(slot):
        t, m = step_of(slot)
        for rows in halves:
            h_ring[lax.rem(slot, 2), rows, :] = b_in[jnp.where(stage > 0, t, 0), m, rows, :].astype(F32) + dot(wlat_t[rows, :], x_in[t, m])

    def attn_norm(slot):
        t, _ = step_of(slot)
        layer_norm(h_ring.at[lax.rem(slot, 2)], u_ref, mid_ref, modb.at[t, 1], modb.at[t, 0])

    def project(part, dst):
        for rows in halves:
            dst[rows, :] = dot(wqkv_t[part * dim + rows.start:part * dim + rows.stop, :], u_ref[...]).astype(BF16)

    def score_dots():
        scores = []
        for hp in range(heads // 2):
            rows = slice(hp * TILE, (hp + 1) * TILE)
            q_pair = q_ref[rows, :]
            k_pair = k_ref[rows, :].T
            for span in tiles:
                q_blk = jnp.concatenate([
                    jnp.concatenate([q_pair[:head_dim, span], zero_q], axis=1),
                    jnp.concatenate([zero_q, q_pair[head_dim:, span]], axis=1)], axis=0)
                full = dot(k_pair[span, :], q_blk)
                scores.append(jnp.where(low_half, full[:head_dim], full[head_dim:]))
        return scores

    def softmax(scores):
        top = jnp.max(scores, axis=0, keepdims=True)
        expd = jnp.exp2((scores - top) * score_scale)
        prob = (expd * (1.0 / jnp.sum(expd, axis=0, keepdims=True))).astype(BF16)
        nought = jnp.zeros_like(prob)
        return jnp.concatenate([jnp.where(low_half, prob, nought), jnp.where(low_half, nought, prob)], axis=0)

    def value_dots(probs):
        for head in range(heads):
            hp, span = head // 2, tiles[head % 2]
            p_blk = jnp.concatenate([
                jnp.concatenate([probs[2 * hp][:, span], zero_p], axis=1),
                jnp.concatenate([zero_p, probs[2 * hp + 1][:, span]], axis=1)], axis=0)
            rows = slice(head * head_dim, (head + 1) * head_dim)
            att_ref[rows, :] = dot(v_ref[rows, :], p_blk).astype(BF16)

    def attn_out(slot):
        t, _ = step_of(slot)
        for rows in halves:
            proj = dot(wo_t[rows, :], att_ref[...])
            for tile in tiles:
                h2_ring[lax.rem(slot, 2), rows, tile] = h_ring[lax.rem(slot, 2), rows, tile] + modb[t, 2, rows, :] * proj[:, tile]

    def mlp_norm(slot):
        t, _ = step_of(slot)
        layer_norm(h2_ring.at[lax.rem(slot, 2)], u2_ref, mid2_ref, modb.at[t, 4], modb.at[t, 3])

    def mlp_up(j):
        rows = slice(j * GROUP, (j + 1) * GROUP)
        half = dot(wup_t[rows, :], u2_ref[...])
        inner = half * (half * half * (8.0 * GELU_A * GELU_B) + 2.0 * GELU_A)
        hid_ref[rows, :] = (half + half * jnp.tanh(inner)).astype(BF16)

    def mlp_down(slot):
        t, m = step_of(slot)
        for rows in halves:
            down = dot(wdown_t[rows, :], hid_ref[...])
            for tile in tiles:
                b_out[t, m, rows, tile] = (h2_ring[lax.rem(slot, 2), rows, tile] + modb[t, 5, rows, :] * down[:, tile]).astype(BF16)

    def latent(slot):
        t, m = step_of(slot)
        eps = dot(wout_ref[...], b_out[t, m])
        x_next = alpha_ref[t] * x_f32[m] + beta_ref[t] * eps
        x_f32[m] = x_next
        x_out[t, m] = x_next.astype(BF16)
        hl_ref[pl.ds(m * tm, tm), :] = b_out[t, m].T

    def receive(slot):
        t, m = step_of(slot)

        @pl.when(jnp.logical_and(t > 0, stage > 0))
        def _():
            h_copy(t - 1, m).wait_recv()

        @pl.when(jnp.logical_and(t > 0, stage < last))
        def _():
            x_copy(t - 1, m, 0).wait_recv()

    def send_stage(slot):
        t, m = step_of(slot)

        @pl.when(jnp.logical_and(t < steps - 1, stage < last))
        def _():
            h_copy(t, m).start()

    def send_latent(slot):
        t, m = step_of(slot)

        @pl.when(jnp.logical_and(t < steps - 1, stage == last))
        def _():
            x_in[t + 1, m] = x_out[t, m]
            for dev in others:
                x_copy(t, m, dev).start()

        @pl.when(jnp.logical_and(t == steps - 1, stage == last))
        def _():
            xo_ref[m] = x_f32[m]
            @pl.when(m == micro - 1)
            def _():
                f_copy(m, x_f32, 0).start()
            for dev in (1, 3, 5, 6):
                f_copy(m, x_f32, dev).start()

    def block(attn=None, out=None, mlp=None, lat=None, extra=None):
        ups = hidden // GROUP
        if attn is not None:
            attn_in(attn)
        if lat is not None:
            latent(lat)
        if mlp is not None:
            for j in range(4):
                mlp_up(j)
        if attn is not None:
            attn_norm(attn)
            project(0, q_ref)
            project(1, k_ref)
        if mlp is not None:
            for j in range(4, ups):
                mlp_up(j)
        if attn is not None:
            scores = score_dots()
            project(2, v_ref)
        if out is not None:
            attn_out(out)
            mlp_norm(out)
        if extra is not None:
            extra()
        if attn is not None:
            value_dots([softmax(s) for s in scores])
        if mlp is not None:
            mlp_down(mlp)
            send_stage(mlp)
        if lat is not None:
            send_latent(lat)

    block(attn=0, extra=late_weights)
    block(attn=1, out=0, extra=late_mods)
    pl.semaphore_wait(barrier, stages - 1)

    def slot_body(slot, carry):
        t, m = step_of(slot)
        receive(slot)
        block(slot, slot - 1, slot - 2, slot - 3)
        return carry
    block(2, 1, 0)
    lax.fori_loop(3, slots, slot_body, 0)
    block(None, slots - 1, slots - 2, slots - 3)
    block(None, None, slots - 1, slots - 2)
    block(None, None, None, slots - 1)

    def whole(src, dst, sem, dev):
        return pltpu.make_async_remote_copy(
            src_ref=src, dst_ref=dst, send_sem=sem, recv_sem=fr_sem.at[0], device_id={'stage': dev}, device_id_type=MESH)

    def relay(part, dev):
        span = pl.ds(0, micro - 1) if part == 0 else pl.ds(micro - 1, 1)
        return pltpu.make_async_remote_copy(
            src_ref=xo_ref.at[span], dst_ref=xo_ref.at[span], send_sem=rs_sem.at[part], recv_sem=fr_sem.at[part],
            device_id={'stage': dev}, device_id_type=MESH)

    sent = pl.ds(0, steps - 1)
    for part in range(2):
        @pl.when(stage < last)
        def _(part=part):
            relay(part, 0).wait_recv()
        for src, dev in ((5, 4), (3, 2), (1, 0)):
            if part == 0 or dev > 0:
                @pl.when(stage == src)
                def _(part=part, dev=dev):
                    relay(part, dev).start()

    @pl.when(stage < last)
    def _():
        whole(b_out.at[sent], b_in.at[pl.ds(1, steps - 1)], hs_sem, jnp.minimum(stage + 1, last)).wait_send()
    for src, dev in ((5, 4), (3, 2), (1, 0)):
        for part in range(2):
            if part == 0 or dev > 0:
                @pl.when(stage == src)
                def _(part=part, dev=dev):
                    relay(part, dev).wait_send()

    @pl.when(stage == last)
    def _():
        for dev in others:
            whole(x_out.at[sent], x_in.at[pl.ds(1, steps - 1)], xs_sem.at[dev], dev).wait_send()
        for dev in (1, 3, 5, 6):
            whole(x_f32, xo_ref, fs_sem.at[dev], dev).wait_send()
        f_copy(micro - 1, x_f32, 0).wait_send()


def solution(mesh):
    stages = mesh.shape['stage']

    def stage_program(x_init, h_warm, w_lat, w_qkv, w_o, w_up, w_down, w_out, ada_mods, alpha_coef, beta_coef):
        batch, tokens, ch = x_init.shape
        total = batch * tokens
        steps, heads, head_dim, dim = ada_mods.shape[0], w_o.shape[1], w_o.shape[2], w_o.shape[3]
        hidden = w_up.shape[2]
        micro, tm = total // GROUP, GROUP
        dims = (steps, stages, heads, head_dim, dim, micro, tm)
        any_spec = pl.BlockSpec(memory_space=pl.ANY)
        vmem_spec = pl.BlockSpec(memory_space=pltpu.VMEM)
        smem_spec = pl.BlockSpec(memory_space=pltpu.SMEM)
        x_out, h_last = pl.pallas_call(
            functools.partial(kernel, dims),
            out_shape=(pltpu.VMEM((micro, ch, tm), F32), pltpu.VMEM((total, dim), BF16)),
            in_specs=[any_spec] * 9 + [smem_spec, smem_spec],
            out_specs=(vmem_spec, vmem_spec),
            scratch_shapes=[
                pltpu.VMEM((ch, dim), BF16), pltpu.VMEM((steps * 6 * dim // TILE, TILE), F32),
                pltpu.VMEM((ch, dim), BF16), pltpu.VMEM((dim, 3 * dim), BF16), pltpu.VMEM((dim, dim), BF16),
                pltpu.VMEM((dim, hidden), BF16), pltpu.VMEM((hidden, dim), BF16),
                pltpu.VMEM((total, dim), BF16), pltpu.VMEM((total, ch), F32),
                pltpu.VMEM((dim, ch), BF16), pltpu.VMEM((3 * dim, dim), BF16), pltpu.VMEM((dim, dim), BF16),
                pltpu.VMEM((hidden, dim), BF16), pltpu.VMEM((dim, hidden), BF16),
                pltpu.VMEM((steps, 6, dim, TILE), F32),
                pltpu.VMEM((dim, tm), F32), pltpu.VMEM((dim, tm), F32), pltpu.VMEM((2, dim, tm), F32), pltpu.VMEM((2, dim, tm), F32),
                pltpu.VMEM((dim, tm), BF16), pltpu.VMEM((dim, tm), BF16),
                pltpu.VMEM((dim, tm), BF16), pltpu.VMEM((dim, tm), BF16), pltpu.VMEM((dim, tm), BF16),
                pltpu.VMEM((dim, tm), BF16), pltpu.VMEM((hidden, tm), BF16),
                pltpu.VMEM((steps, micro, dim, tm), BF16), pltpu.VMEM((steps, micro, ch, tm), BF16),
                pltpu.VMEM((steps, micro, dim, tm), BF16), pltpu.VMEM((steps, micro, ch, tm), BF16), pltpu.VMEM((micro, ch, tm), F32),
                pltpu.SemaphoreType.DMA((9,)),
                pltpu.SemaphoreType.DMA, pltpu.SemaphoreType.DMA((steps - 1, micro)),
                pltpu.SemaphoreType.DMA((stages,)), pltpu.SemaphoreType.DMA((steps - 1, micro)),
                pltpu.SemaphoreType.DMA((stages,)), pltpu.SemaphoreType.DMA((2,)), pltpu.SemaphoreType.DMA((2,)),
            ],
            compiler_params=pltpu.CompilerParams(collective_id=0, has_side_effects=True, vmem_limit_bytes=60 * 1024 * 1024),
        )(x_init.reshape(total, ch), h_warm.reshape(stages - 1, total, dim), w_lat.reshape(ch, dim),
          w_qkv.reshape(dim, 3 * dim), w_o.reshape(heads * head_dim, dim), w_up.reshape(dim, hidden),
          w_down.reshape(hidden, dim), w_out.T, ada_mods.reshape(steps * 6 * dim // TILE, TILE), alpha_coef, beta_coef)
        x_out = x_out.transpose(0, 2, 1)
        return x_out.reshape(batch, tokens, ch), h_last.reshape(1, batch, tokens, dim)

    return jax.shard_map(stage_program, mesh=mesh,
                         in_specs=(P('data'), P(None, 'data'), P('stage'), P('stage'), P('stage'), P('stage'), P('stage'), P(), P(None, 'stage'), P(), P()),
                         out_specs=(P('data'), P('stage', 'data')), check_vma=False)
```
